512 devices in a mesh: expert: 8 (over x, z_hi), tensor: 64 (over y, z_lo, core).
Axes of the slice: x: 4, y: 8, z: 8 (z_hi: 2, z_lo: 4; z = z_hi * 4 + z_lo), core: 2. Of those that a mesh axis runs over, the one named last changes fastest.
Arguments:
- tokens: bfloat16 [384, 6144], P('expert', 'tensor'), may hold values from -6 to 6
- expert_ids: int32 [384, 2], P('expert'), may hold values from 0 to 7, as said below
- route_weight: int32 [384, 2], P('expert'), may hold values from 1 to 4095
- gate_weight: bfloat16 [8, 6144, 8192], P('expert', None, 'tensor'), may hold values from -0.078125 to 0.078125
- up_weight: bfloat16 [8, 6144, 8192], P('expert', None, 'tensor'), may hold values from -0.078125 to 0.078125
- down_weight: bfloat16 [8, 8192, 6144], P('expert', 'tensor'), may hold values from -0.0625 to 0.0625
Outputs:
- mixed: bfloat16 [384, 6144], P('expert', 'tensor')
- expert_load: float32 [2, 8], replicated
The draws below stay inside these ranges and needn't reach their ends.
Inputs may be any that keep to these rules, and one draw needn't show every extreme that they name: `expert_ids`: each row names two different experts. The hot expert is the one named in the first column of the first row of every aligned block of 48 rows (the tokens of one expert group), the same in all blocks. In each block exactly 42 rows name the hot expert, in either column; every other expert is named by 7 or 8 rows of each block, and by exactly 8 rows in some.
All inputs are finite; a program needn't handle non-finite values.
Results may differ from the reference program's by a relative error of at most 0.005.
Values may be sent and summed in bfloat16 or wider, within the bound.
A program may use at most 64 MiB of HBM per device.

```python
import jax
import jax.numpy as jnp
from jax import lax

D = 6144
FF = 8192
TOK_DEV = 48
EXPERTS = 8
TOKENS = 384
HOT_ROWS = 42
CAP = 8


def draw_expert_ids(key, part):
    hot_id = jax.random.randint(jax.random.fold_in(key, 101), (1,), 0, EXPERTS).astype(jnp.int32)[0]
    block_count = TOKENS // TOK_DEV
    cold_count = EXPERTS - 1
    scores = jax.random.randint(jax.random.fold_in(key, 202), (block_count, TOK_DEV), 0, 1048576).astype(jnp.int32)
    scores = scores * TOK_DEV + jnp.arange(TOK_DEV, dtype=jnp.int32)[None, :]
    scores = jnp.where(jnp.arange(TOK_DEV, dtype=jnp.int32)[None, :] == 0, jnp.int32(-1), scores)
    order = jnp.argsort(scores, axis=1, stable=True).astype(jnp.int32)
    rank = jnp.argsort(order, axis=1, stable=True).astype(jnp.int32)
    rotation = jax.random.randint(jax.random.fold_in(key, 303), (block_count, 1), 0, cold_count).astype(jnp.int32)
    first_slot = jnp.where(rank < HOT_ROWS, rank, HOT_ROWS + 2 * (rank - HOT_ROWS))
    second_slot = jnp.where(rank < HOT_ROWS, rank, first_slot + 1)

    def cold_label(slot_number):
        shifted = (slot_number + rotation) % cold_count
        return shifted + (shifted >= hot_id).astype(jnp.int32)
    first = jnp.where(rank < HOT_ROWS, hot_id, cold_label(first_slot))
    second = cold_label(second_slot)
    flips = jax.random.randint(jax.random.fold_in(key, 404), (block_count, TOK_DEV), 0, 2).astype(jnp.int32)
    flips = jnp.where(jnp.arange(TOK_DEV, dtype=jnp.int32)[None, :] == 0, jnp.int32(0), flips)
    left = jnp.where(flips == 1, second, first)
    right = jnp.where(flips == 1, first, second)
    return jnp.stack([left, right], axis=2).reshape(TOKENS, 2).astype(jnp.int32)


def place_ends(array, key, low, top_value):
    spot = [jax.random.randint(jax.random.fold_in(key, axis), (), 0, length) for axis, length in enumerate(array.shape)]
    longest = array.shape.index(max(array.shape))
    neighbour = spot[:longest] + [(spot[longest] + 1) % array.shape[longest]] + spot[longest + 1:]
    return array.at[tuple(spot)].set(low).at[tuple(neighbour)].set(top_value)


def levels(key, shape, split, smallest, high):
    loudness = 1.0
    for position, parts in split:
        steps = jax.random.uniform(jax.random.fold_in(jax.random.fold_in(key, 6), position), (parts,), jnp.float32, smallest / len(split), high / len(split))
        loudness = loudness * jnp.repeat(jnp.exp(steps), shape[position] // parts).reshape((-1,) + (1,) * (len(shape) - 1 - position))
    return loudness


def centred(own_key, shape, deviation, reach, pieces=(), held_as=jnp.bfloat16):
    values = jax.random.normal(own_key, shape, jnp.float32) * deviation
    if len(pieces) > 0:
        values = levels(own_key, shape, pieces, -0.22, 0.18) * values
    return jnp.clip(values, min=-reach, max=reach).astype(held_as)


def setup_inputs(seed: int = 0) -> dict:
    streams_of = jax.random.split(jax.random.key(seed), 7)
    return {
        "tokens": centred(streams_of[0], (TOKENS, D), 1.0, 6.0, ((0, 8), (1, 64))),
        "expert_ids": draw_expert_ids(jax.random.fold_in(streams_of[6], 71), 0),
        "route_weight": place_ends(jax.random.randint(streams_of[2], (TOKENS, 2), 1, 4096), jax.random.fold_in(streams_of[2], 1), 1, 4095).astype(jnp.int32),
        "gate_weight": centred(streams_of[3], (EXPERTS, D, FF), D ** -0.5, 0.078125, ((0, 8), (2, 64))),
        "up_weight": centred(streams_of[4], (EXPERTS, D, FF), D ** -0.5, 0.078125, ((0, 8), (2, 64))),
        "down_weight": centred(streams_of[5], (EXPERTS, FF, D), FF ** -0.5, 0.0625, ((0, 8), (1, 64))),
    }


def expert_ffn(row_block, w_gate, w_up, w_down):
    gate_value = jnp.dot(row_block, w_gate, preferred_element_type=jnp.float32)
    up_value = jnp.dot(row_block, w_up, preferred_element_type=jnp.float32)
    hidden = (jax.nn.silu(gate_value) * up_value).astype(jnp.bfloat16)
    return jnp.dot(hidden, w_down, preferred_element_type=jnp.float32)


def reference(tokens, expert_ids, route_weight, gate_weight, up_weight, down_weight):
    weights = route_weight.astype(jnp.float32)
    route_share = weights / jnp.sum(weights, axis=1, keepdims=True)
    labels = jnp.arange(EXPERTS, dtype=jnp.int32)
    chosen = expert_ids[:, :, None] == labels[None, None, :]
    mixing = jnp.sum(jnp.where(chosen, route_share[:, :, None], jnp.float32(0.0)), axis=1)
    hot_id = expert_ids[0, 0]

    def add_rows(running, row_mask, most_rows, expert):
        row_index = jnp.nonzero(row_mask, size=most_rows, fill_value=0)[0].astype(jnp.int32)
        counted = jnp.sum(row_mask.astype(jnp.int32))
        is_valid = jnp.arange(most_rows, dtype=jnp.int32) < counted
        expert_out = expert_ffn(tokens[row_index], gate_weight[expert], up_weight[expert], down_weight[expert])
        row_scale = jnp.where(is_valid, mixing[row_index, expert], jnp.float32(0.0))
        return running.at[row_index].add(row_scale[:, None] * expert_out)

    running = jnp.zeros((TOKENS, D), jnp.float32)
    hot_mask = jnp.any(expert_ids == hot_id, axis=1)
    running = add_rows(running, hot_mask, EXPERTS * HOT_ROWS, hot_id)

    def cold_step(carry, expert):
        cold_mask = jnp.any(expert_ids == expert, axis=1) & (expert != hot_id)
        return add_rows(carry, cold_mask, EXPERTS * CAP, expert), None

    running, unused = lax.scan(cold_step, running, labels)
    counts = jnp.sum(chosen.astype(jnp.float32), axis=(0, 1))
    expert_load = jnp.stack([counts, jnp.sum(mixing, axis=0)]) / TOK_DEV
    return running.astype(jnp.bfloat16), expert_load
```

```python
import jax
import jax.numpy as jnp
from jax import lax
from jax.experimental import pallas as pl
from jax.experimental.pallas import tpu as pltpu
from jax.sharding import PartitionSpec as P

MESH = pl.DeviceIdType.MESH
F32 = jnp.float32
BF16 = jnp.bfloat16
RING = 8


def kernel(
    tok_ref, ids_ref, raw_ref, gate_ref, up_ref, down_ref,
    out_ref, load_ref,
    near, square, tabs, first, blocks, wk, dn, dk, acc, hid, scl,
    sent, came, own32, own16, direct, last_out, last_in,
    w_sem, d_sem, x_send, x_recv, t_send, t_recv, f_send, f_recv,
    a_send, a_recv, r_send, r_recv, l_send, l_recv, o_send, o_recv,
):
    e = lax.axis_index("expert")
    t = lax.axis_index("tensor")
    x, z_hi = e // 2, e % 2
    y, z_lo, c = t // 8, (t // 2) % 4, t % 2
    z = z_hi * 4 + z_lo
    half = x // 2
    p1 = z + c * (y - z)
    p2 = y + c * (z - y)

    def device(x_, y_, z_, c_):
        return (x_ * 2 + z_ // 4, (y_ * 4 + z_ % 4) * 2 + c_)

    def on_rings(a, b):
        return device(x, b + c * (a - b), a + c * (b - a), c)

    def remote(src, dst, send, recv, target):
        return pltpu.make_async_remote_copy(
            src_ref=src, dst_ref=dst, send_sem=send, recv_sem=recv,
            device_id=target, device_id_type=MESH,
        )

    sibling = device(x, y, z, 1 - c)

    def weight_rows(i, path):
        kb, j = i // 4, i % 4
        straight = kb * 768 + j * 192
        across = ((kb % 2) * 4 + j) * 768 + (kb // 2) * 192
        return pl.ds(pl.multiple_of(straight + path * (across - straight), 64), 192)

    def weight_slot(i, k):
        return wk.at[i // 4, pl.ds(pl.multiple_of((i % 4) * 192, 64), 192), pl.ds(pl.multiple_of(k * 128, 128), 128)]

    def local_weights(i, carry):
        rows = weight_rows(i, c)
        pltpu.make_async_copy(gate_ref.at[0, rows, :], weight_slot(i, c), w_sem.at[0]).start()
        pltpu.make_async_copy(up_ref.at[0, rows, :], weight_slot(i, 2 + c), w_sem.at[1]).start()
        return carry

    lax.fori_loop(0, 32, local_weights, 0)
    own_down = dn.at[pl.ds(pl.multiple_of(c * 128, 128), 128), :]
    their_down = dn.at[pl.ds(pl.multiple_of((1 - c) * 128, 128), 128), :]
    pltpu.make_async_copy(down_ref.at[0], own_down, d_sem.at[0]).start()

    barrier = pltpu.get_barrier_semaphore()

    def greet(target):
        pl.semaphore_signal(barrier, inc=1, device_id=target, device_id_type=MESH)

    for k in range(1, RING):
        other = (x * 2 + c + k) % 8
        greet(device(other // 2, y, z, other % 2))
        greet(on_rings((p1 + k) % RING, p2))
    for k in (1, 4, 7):
        greet(on_rings(p1, (p2 + k) % RING))

    lane = lax.broadcasted_iota(jnp.int32, (48, 128), 1)
    weights = raw_ref[...].astype(F32)
    share = weights / (weights[:, 0:1] + weights[:, 1:2])
    ids = ids_ref[...]
    hit0 = ids[:, 0:1] == lane
    hit1 = ids[:, 1:2] == lane
    zero = jnp.zeros((48, 128), F32)
    mix = jnp.where(hit0, share[:, 0:1], zero) + jnp.where(hit1, share[:, 1:2], zero)
    hits = jnp.where(hit0, 1.0, 0.0) + jnp.where(hit1, 1.0, 0.0)
    square[...] = jnp.zeros((128, 128), F32)
    square[0:48, :] = mix
    square[48:49, :] = jnp.sum(hits, axis=0, keepdims=True)
    square[49:50, :] = jnp.sum(mix, axis=0, keepdims=True)
    tabs[z_hi, x] = jnp.transpose(square[...])[0:8, :]

    pl.semaphore_wait(barrier, 17)

    for d in (2, 1, 3):
        remote(
            tok_ref, near.at[x % 2, c], x_send.at[d], x_recv.at[x % 2, c],
            device((x + d) % 4, y, z, half),
        ).start()

    @pl.when(half != c)
    def _():
        remote(tok_ref, near.at[x % 2, c], x_send.at[0], x_recv.at[x % 2, c], sibling).start()

    @pl.when(half == c)
    def _():
        near[x % 2, c] = tok_ref[...]

    table = lambda d: remote(
        tabs.at[z_hi, x], tabs.at[z_hi, x], t_send.at[d], t_recv.at[d],
        device((x + d) % 4, y, z, c),
    )
    for d in (1, 2, 3):
        table(d).start()

    def remote_weights(i, carry):
        rows = weight_rows(i, 1 - c)
        remote(gate_ref.at[0, rows, :], weight_slot(i, c), w_sem.at[2], w_sem.at[4], sibling).start()
        remote(up_ref.at[0, rows, :], weight_slot(i, 2 + c), w_sem.at[3], w_sem.at[5], sibling).start()
        return carry

    lax.fori_loop(0, 32, remote_weights, 0)
    down_copy = remote(down_ref.at[0], own_down, d_sem.at[1], d_sem.at[2], sibling)
    down_copy.start()

    for xh in range(2):
        for cs in range(2):
            @pl.when((2 * c + xh != x) | (c != cs))
            def _():
                remote(
                    tok_ref, near.at[xh, cs], x_send.at[0], x_recv.at[xh, cs], sibling
                ).wait_recv()

    pieces = [near[xh, cs].astype(F32) for xh in range(2) for cs in range(2)]
    first[p1] = jnp.concatenate(pieces, axis=1).astype(BF16)

    around = lambda k: remote(
        first.at[p1], first.at[p1], f_send.at[k], f_recv.at[k], on_rings((p1 + k) % RING, p2)
    )
    for k in (4, 3, 5, 2, 6, 1, 7):
        around(k).start()
    for d in (1, 2, 3):
        remote(
            tabs.at[z_hi, x], tabs.at[z_hi, (x + 4 - d) % 4], t_send.at[d], t_recv.at[d], sibling
        ).wait_recv()
    mirror = device(x, y, (z + 4) % 8, c)
    far_table = remote(tabs.at[z_hi], tabs.at[z_hi], t_send.at[0], t_recv.at[0], mirror)
    far_table.start()

    acc[...] = jnp.zeros_like(acc)
    for k in (1, 7, 2, 6, 3, 5, 4):
        remote(
            first.at[p1], first.at[(p1 + RING - k) % RING], f_send.at[k], f_recv.at[k], sibling
        ).wait_recv()

    def ring_copy(way, step, b, sub):
        target = on_rings(p1, (p2 + (1 if way == 0 else 7)) % RING)
        return remote(
            blocks.at[b, sub], blocks.at[b, sub],
            a_send.at[way, step, sub], a_recv.at[way, step, sub], target,
        )

    for h in range(2):
        for xh in range(2):
            sub = h * 2 + xh
            parts = [first[h * 4 + lo][:, xh * 192:(xh + 1) * 192].astype(F32) for lo in range(4)]
            blocks[p2, sub] = jnp.concatenate(parts, axis=1).astype(BF16)
            ring_copy(0, 0, p2, sub).start()
            ring_copy(1, 0, p2, sub).start()

    def place(b, h):
        across = (b % 4) * 2 + h
        return b + c * (across - b), h + c * (b // 4 - h)

    def project(b, h):
        kb, r = place(b, h)
        rows = blocks[b, pl.ds(2 * h, 2)].reshape(96, 768)
        acc[r] += jnp.dot(rows, wk[kb], preferred_element_type=F32)

    for k in range(2):
        mine = wk.at[:, :, pl.ds(pl.multiple_of((2 * k + c) * 128, 128), 128)]
        theirs = wk.at[:, :, pl.ds(pl.multiple_of((2 * k + 1 - c) * 128, 128), 128)]
        pltpu.make_async_copy(mine, mine, w_sem.at[k]).wait()
        pltpu.make_async_copy(theirs, theirs, w_sem.at[4 + k]).wait()
    project(p2, 0)
    project(p2, 1)
    pltpu.make_async_copy(down_ref.at[0], own_down, d_sem.at[0]).wait()
    pltpu.make_async_copy(down_ref.at[0], their_down, d_sem.at[2]).wait()

    @pl.when(c == 0)
    def _():
        for kb in range(8):
            dk[kb] = dn[:, kb * 768:(kb + 1) * 768]

    @pl.when(c == 1)
    def _():
        def repack(g, carry):
            rows = pl.ds(pl.multiple_of(g * 32, 32), 32)
            for kb in range(8):
                lo, hi = kb // 2, kb % 2
                cuts = [
                    dn[rows, (hi * 4 + j) * 768 + lo * 192:(hi * 4 + j) * 768 + (lo + 1) * 192].astype(F32)
                    for j in range(4)
                ]
                dk[kb, rows, :] = jnp.concatenate(cuts, axis=1).astype(BF16)
            return carry

        lax.fori_loop(0, 8, repack, 0)

    def gather_step(r, carry):
        held = ((p2 + RING - r) % RING, (p2 + r) % RING)
        for h in range(2):
            for xh in range(2):
                sub = h * 2 + xh
                for way in range(2):
                    ring_copy(way, r - 1, held[way], sub).wait_recv()
                    if h == way:
                        ring_copy(way, r, held[way], sub).start()
                    else:
                        @pl.when(r < 3)
                        def _():
                            ring_copy(way, r, held[way], sub).start()
            for way in range(2):
                project(held[way], h)
        return carry

    lax.fori_loop(1, 4, gather_step, 0)
    far = (p2 + 4) % RING
    for xh in range(2):
        for way in range(2):
            ring_copy(way, 3, far, way * 2 + xh).wait_recv()
    for way in range(2):
        project(far, way)

    remote(tabs.at[z_hi], tabs.at[1 - z_hi], t_send.at[0], t_recv.at[0], mirror).wait_recv()
    lane96 = lax.broadcasted_iota(jnp.int32, (128, 8), 1)
    for r in range(2):
        for xh in range(2):
            turned = jnp.transpose(tabs[r, 2 * c + xh])
            picked = jnp.sum(jnp.where(lane96 == e, turned, 0.0), axis=1, keepdims=True)
            scl[r, xh * 48:(xh + 1) * 48, :] = jnp.broadcast_to(picked[0:48], (48, 128))
        gate = acc[r, :, 0:256]
        up = acc[r, :, 256:512]
        hid[r] = (gate / (1.0 + jnp.exp(-gate)) * up).astype(BF16)
    everyone = tabs[0, 0]
    for k in range(1, 8):
        everyone = everyone + tabs[k // 4, k % 4]
    load_ref[...] = jnp.transpose(everyone)[48:50, :] / 48.0

    def own_part(q, h):
        kb, r = place(q, h)
        part = jnp.dot(hid[r], dk[kb], preferred_element_type=F32)
        return part * scl[r][:, 0:1]

    def sum_copy(way, s, sub):
        target = on_rings(p1, (p2 + (1 if way == 0 else 7)) % RING)
        return remote(
            sent.at[way, s, sub], came.at[way, s, sub],
            r_send.at[way, s, sub], r_recv.at[way, s, sub], target,
        )

    def pass_on(s, h, way, has_come):
        q = (p2 + (4 - s if way == 0 else 4 + s)) % RING
        part = own_part(q, h)
        for xh in range(2):
            sub = h * 2 + xh
            value = part[xh * 48:(xh + 1) * 48]
            if has_come:
                sum_copy(way, s - 1, sub).wait_recv()
                value = value + came[way, s - 1, sub].astype(F32)
            sent[way, s, sub] = value.astype(BF16)
            sum_copy(way, s, sub).start()

    for way in range(2):
        pass_on(0, way, way, False)
    for way in range(2):
        pass_on(1, 1 - way, way, False)
    for way in range(2):
        pass_on(1, way, way, True)

    def sum_step(s, carry):
        for way in range(2):
            pass_on(s, 1 - way, way, True)
        for way in range(2):
            pass_on(s, way, way, True)
        return carry

    lax.fori_loop(2, 4, sum_step, 0)

    scatter = lambda k: remote(
        own16.at[(p1 + k) % RING], direct.at[k], l_send.at[k], l_recv.at[k],
        on_rings((p1 + k) % RING, p2),
    )
    for h in range(2):
        part = own_part(p2, h)
        halves = []
        for xh in range(2):
            sub = h * 2 + xh
            value = part[xh * 48:(xh + 1) * 48]
            for way in range(2):
                sum_copy(way, 3, sub).wait_recv()
                value = value + came[way, 3, sub].astype(F32)
            halves.append(value)
        for lo in range(4):
            both = jnp.concatenate([v[:, lo * 192:(lo + 1) * 192] for v in halves], axis=1)
            own32[h * 4 + lo] = both
            own16[h * 4 + lo] = both.astype(BF16)
    for k in (4, 3, 5, 2, 6, 1, 7):
        scatter(k).start()
    total = own32[p1]
    for k in (1, 7, 2, 6, 3, 5, 4):
        scatter(k).wait_recv()
        total = total + direct[k].astype(F32)
    for xt in range(2):
        for ct in range(2):
            last_out[xt, ct] = total[:, xt * 192 + ct * 96:xt * 192 + (ct + 1) * 96]

    def home(xt, ct):
        return remote(
            last_out.at[xt, ct], last_in.at[x], o_send.at[xt, ct], o_recv.at[x],
            device(2 * c + xt, y, z, ct),
        )

    for xt in range(2):
        for ct in range(2):
            @pl.when((2 * c + xt != x) | (c != ct))
            def _():
                home(xt, ct).start()

    @pl.when(half == c)
    def _():
        last_in[x] = last_out[x % 2, c]

    for xs in range(4):
        @pl.when((xs != x) | (half != c))
        def _():
            remote(
                last_out.at[0, 0], last_in.at[xs], o_send.at[0, 0], o_recv.at[xs], sibling
            ).wait_recv()
    out_ref[...] = (last_in[0] + last_in[1] + last_in[2] + last_in[3]).astype(BF16)

    for xt in range(2):
        for ct in range(2):
            @pl.when((2 * c + xt != x) | (c != ct))
            def _():
                home(xt, ct).wait_send()
    for k in range(1, RING):
        scatter(k).wait_send()
        around(k).wait_send()
    for d in (1, 2, 3):
        table(d).wait_send()
        remote(
            tok_ref, near.at[x % 2, c], x_send.at[d], x_recv.at[x % 2, c],
            device((x + d) % 4, y, z, half),
        ).wait_send()

    @pl.when(half != c)
    def _():
        remote(tok_ref, near.at[x % 2, c], x_send.at[0], x_recv.at[x % 2, c], sibling).wait_send()

    far_table.wait_send()
    down_copy.wait_send()
    for k in range(2):
        mine = wk.at[:, :, pl.ds(pl.multiple_of((2 * k + c) * 128, 128), 128)]
        pltpu.make_async_copy(mine, mine, w_sem.at[2 + k]).wait()

    def left(s, carry):
        for way in range(2):
            for sub in range(4):
                ring_copy(way, s, p2, sub).wait_send()
                sum_copy(way, s + 1, sub).wait_send()
        return carry

    lax.fori_loop(0, 3, left, 0)
    for way in range(2):
        for xh in range(2):
            ring_copy(way, 3, p2, way * 2 + xh).wait_send()
            sum_copy(way, 0, way * 2 + xh).wait_send()


def local(tokens, expert_ids, route_weight, gate_weight, up_weight, down_weight):
    vmem, dma = pltpu.VMEM, pltpu.SemaphoreType.DMA
    inside = pl.BlockSpec(memory_space=pltpu.VMEM)
    outside = pl.BlockSpec(memory_space=pl.ANY)
    return pl.pallas_call(
        kernel,
        name="layer",
        out_shape=(
            jax.ShapeDtypeStruct((48, 96), BF16),
            jax.ShapeDtypeStruct((2, 8), F32),
        ),
        in_specs=[inside] * 3 + [outside] * 3,
        out_specs=(inside, inside),
        scratch_shapes=[
            vmem((2, 2, 48, 96), BF16),
            vmem((128, 128), F32),
            vmem((2, 4, 8, 128), F32),
            vmem((8, 48, 384), BF16),
            vmem((8, 4, 48, 768), BF16),
            vmem((8, 768, 512), BF16),
            vmem((256, 6144), BF16),
            vmem((8, 256, 768), BF16),
            vmem((2, 96, 512), F32),
            vmem((2, 96, 256), BF16),
            vmem((2, 96, 128), F32),
            vmem((2, 4, 4, 48, 768), BF16),
            vmem((2, 4, 4, 48, 768), BF16),
            vmem((8, 48, 384), F32),
            vmem((8, 48, 384), BF16),
            vmem((8, 48, 384), BF16),
            vmem((2, 2, 48, 96), F32),
            vmem((4, 48, 96), F32),
            dma((6,)),
            dma((3,)),
            dma((4,)),
            dma((2, 2)),
            dma((4,)),
            dma((4,)),
            dma((8,)),
            dma((8,)),
            dma((2, 4, 4)),
            dma((2, 4, 4)),
            dma((2, 4, 4)),
            dma((2, 4, 4)),
            dma((8,)),
            dma((8,)),
            dma((2, 2)),
            dma((4,)),
        ],
        compiler_params=pltpu.CompilerParams(
            collective_id=0, has_side_effects=True, vmem_limit_bytes=48 * 1024 * 1024
        ),
    )(tokens, expert_ids, route_weight, gate_weight, up_weight, down_weight)


def solution(mesh):
    placed = (
        P("expert", "tensor"),
        P("expert", None),
        P("expert", None),
        P("expert", None, "tensor"),
        P("expert", None, "tensor"),
        P("expert", "tensor", None),
    )
    return jax.shard_map(
        local, mesh=mesh, in_specs=placed, out_specs=(P("expert", "tensor"), P()), check_vma=False
    )
```

```python
import jax
import jax.numpy as jnp
from jax import lax
from jax.experimental import pallas as pl
from jax.experimental.pallas import tpu as pltpu
from jax.sharding import PartitionSpec as P

MESH = pl.DeviceIdType.MESH
F32 = jnp.float32
BF16 = jnp.bfloat16
RING = 8


def kernel(
    tok_hbm, ids_hbm, raw_hbm, gate_ref, up_ref, down_ref,
    out_ref, load_ref,
    tok_ref, ids_ref, raw_ref, near, tabs, first, blocks, wk, dn, dk, acc, hid, scl, ahead,
    sent, came, own32, own16, direct, last_out, last_in,
    in_sem, w_sem, d_sem, x_send, x_recv, t_send, t_recv, f_send, f_recv,
    a_send, a_recv, r_send, r_recv, l_send, l_recv, o_send, o_recv, pair_sem,
):
    e = lax.axis_index("expert")
    t = lax.axis_index("tensor")
    x, z_hi = e // 2, e % 2
    y, z_lo, c = t // 8, (t // 2) % 4, t % 2
    z = z_hi * 4 + z_lo
    half = x // 2
    p1 = z + c * (y - z)
    p2 = y + c * (z - y)

    def device(x_, y_, z_, c_):
        return (x_ * 2 + z_ // 4, (y_ * 4 + z_ % 4) * 2 + c_)

    def on_rings(a, b):
        return device(x, b + c * (a - b), a + c * (b - a), c)

    def remote(src, dst, send, recv, target):
        return pltpu.make_async_remote_copy(
            src_ref=src, dst_ref=dst, send_sem=send, recv_sem=recv,
            device_id=target, device_id_type=MESH,
        )

    sibling = device(x, y, z, 1 - c)

    barrier = pltpu.get_barrier_semaphore()

    def greet(target):
        pl.semaphore_signal(barrier, inc=1, device_id=target, device_id_type=MESH)

    for k in range(1, RING):
        other = (x * 2 + c + k) % 8
        greet(device(other // 2, y, z, other % 2))
        greet(on_rings((p1 + k) % RING, p2))
    for k in (1, 4, 7):
        greet(on_rings(p1, (p2 + k) % RING))

    def weight_rows(i, path):
        kb, j = i // 4, i % 4
        straight = kb * 768 + j * 192
        across = ((kb % 2) * 4 + j) * 768 + (kb // 2) * 192
        return pl.ds(pl.multiple_of(straight + path * (across - straight), 64), 192)

    def weight_slot(i, k):
        return wk.at[i // 4, pl.ds(pl.multiple_of((i % 4) * 192, 64), 192), pl.ds(pl.multiple_of(k * 128, 128), 128)]

    def local_weights(i, carry):
        rows = weight_rows(i, c)
        pltpu.make_async_copy(gate_ref.at[0, rows, :], weight_slot(i, c), w_sem.at[0]).start()
        pltpu.make_async_copy(up_ref.at[0, rows, :], weight_slot(i, 2 + c), w_sem.at[1]).start()
        return carry

    tok_copy = pltpu.make_async_copy(tok_hbm, tok_ref, in_sem.at[0])
    ids_copy = pltpu.make_async_copy(ids_hbm, ids_ref, in_sem.at[1])
    raw_copy = pltpu.make_async_copy(raw_hbm, raw_ref, in_sem.at[2])
    tok_copy.start()
    ids_copy.start()
    raw_copy.start()
    own_down = dn.at[pl.ds(pl.multiple_of(c * 128, 128), 128), :]
    their_down = dn.at[pl.ds(pl.multiple_of((1 - c) * 128, 128), 128), :]
    pltpu.make_async_copy(down_ref.at[0], own_down, d_sem.at[0]).start()

    lax.fori_loop(0, 32, local_weights, 0)

    ids_copy.wait()
    raw_copy.wait()
    row = lax.broadcasted_iota(jnp.int32, (8, 48), 0)
    weights = raw_ref[...].astype(F32)
    share = weights / (weights[0:1, :] + weights[1:2, :])
    ids = ids_ref[...]
    zero = jnp.zeros((8, 48), F32)
    hit0 = ids[0:1, :] == row
    hit1 = ids[1:2, :] == row
    mix = jnp.where(hit0, share[0:1, :], zero) + jnp.where(hit1, share[1:2, :], zero)
    hits = jnp.where(hit0, 1.0, zero) + jnp.where(hit1, 1.0, zero)
    tabs[z_hi, x, :, 0:48] = mix
    tabs[z_hi, x, :, 48:128] = jnp.where(
        lax.broadcasted_iota(jnp.int32, (8, 80), 1) == 0,
        jnp.sum(hits, axis=1, keepdims=True), jnp.sum(mix, axis=1, keepdims=True),
    )

    tok_copy.wait()
    pl.semaphore_wait(barrier, 17)

    for d in (2, 1, 3):
        remote(
            tok_ref, near.at[x % 2, c], x_send.at[d], x_recv.at[x % 2, c],
            device((x + d) % 4, y, z, half),
        ).start()

    @pl.when(half != c)
    def _():
        remote(tok_ref, near.at[x % 2, c], x_send.at[0], x_recv.at[x % 2, c], sibling).start()

    @pl.when(half == c)
    def _():
        near[x % 2, c] = tok_ref[...]

    table = lambda d: remote(
        tabs.at[z_hi, x], tabs.at[z_hi, x], t_send.at[d], t_recv.at[d],
        device((x + d) % 4, y, z, c),
    )
    for d in (1, 2, 3):
        table(d).start()

    def remote_weights(i, carry):
        rows = weight_rows(i, 1 - c)
        remote(gate_ref.at[0, rows, :], weight_slot(i, c), w_sem.at[2], w_sem.at[4], sibling).start()
        remote(up_ref.at[0, rows, :], weight_slot(i, 2 + c), w_sem.at[3], w_sem.at[5], sibling).start()
        return carry

    lax.fori_loop(0, 32, remote_weights, 0)
    down_copy = remote(down_ref.at[0], own_down, d_sem.at[1], d_sem.at[2], sibling)
    down_copy.start()

    for xh in range(2):
        for cs in range(2):
            @pl.when((2 * c + xh != x) | (c != cs))
            def _():
                remote(
                    tok_ref, near.at[xh, cs], x_send.at[0], x_recv.at[xh, cs], sibling
                ).wait_recv()

    pieces = [near[xh, cs].astype(F32) for xh in range(2) for cs in range(2)]
    first[p1] = jnp.concatenate(pieces, axis=1).astype(BF16)

    around = lambda k: remote(
        first.at[p1], first.at[p1], f_send.at[0], f_recv.at[k], on_rings((p1 + k) % RING, p2)
    )
    for k in (4, 3, 5, 2, 6, 1, 7):
        around(k).start()
    for d in (1, 2, 3):
        remote(
            tabs.at[z_hi, x], tabs.at[z_hi, (x + 4 - d) % 4], t_send.at[d], t_recv.at[d], sibling
        ).wait_recv()
    mirror = device(x, y, (z + 4) % 8, c)
    far_table = remote(tabs.at[z_hi], tabs.at[z_hi], t_send.at[0], t_recv.at[0], mirror)
    far_table.start()

    acc[...] = jnp.zeros_like(acc)
    for k in (1, 7, 2, 6, 3, 5, 4):
        remote(
            first.at[p1], first.at[(p1 + RING - k) % RING], f_send.at[0], f_recv.at[k], sibling
        ).wait_recv()

    def ring_copy(way, step, b, sub):
        target = on_rings(p1, (p2 + (1 if way == 0 else 7)) % RING)
        return remote(
            blocks.at[b, sub], blocks.at[b, sub],
            a_send.at[0], a_recv.at[way, step, sub], target,
        )

    for h in range(2):
        for xh in range(2):
            for lh in range(2):
                sub = h * 4 + xh * 2 + lh
                parts = [
                    first[h * 4 + lh * 2 + lo][:, xh * 192:(xh + 1) * 192].astype(F32)
                    for lo in range(2)
                ]
                blocks[p2, sub] = jnp.concatenate(parts, axis=1).astype(BF16)
                ring_copy(0, 0, p2, sub).start()
                ring_copy(1, 0, p2, sub).start()

    def place(b, h):
        across = (b % 4) * 2 + h
        return b + c * (across - b), h + c * (b // 4 - h)

    def project(b, h):
        kb, r = place(b, h)
        part = blocks[b, pl.ds(4 * h, 4)]
        rows = jnp.concatenate(
            [jnp.concatenate([part[2 * xh], part[2 * xh + 1]], axis=1) for xh in range(2)], axis=0
        )
        acc[r] += jnp.dot(rows, wk[kb], preferred_element_type=F32)

    for k in range(2):
        mine = wk.at[:, :, pl.ds(pl.multiple_of((2 * k + c) * 128, 128), 128)]
        theirs = wk.at[:, :, pl.ds(pl.multiple_of((2 * k + 1 - c) * 128, 128), 128)]
        pltpu.make_async_copy(mine, mine, w_sem.at[k]).wait()
        pltpu.make_async_copy(theirs, theirs, w_sem.at[4 + k]).wait()
    project(p2, 0)
    project(p2, 1)
    pltpu.make_async_copy(down_ref.at[0], own_down, d_sem.at[0]).wait()
    pltpu.make_async_copy(down_ref.at[0], their_down, d_sem.at[2]).wait()

    @pl.when(c == 0)
    def _():
        for kb in range(8):
            dk[kb] = dn[:, kb * 768:(kb + 1) * 768]

    @pl.when(c == 1)
    def _():
        def repack(g, carry):
            rows = pl.ds(pl.multiple_of(g * 32, 32), 32)
            for kb in range(8):
                lo, hi = kb // 2, kb % 2
                cuts = [
                    dn[rows, (hi * 4 + j) * 768 + lo * 192:(hi * 4 + j) * 768 + (lo + 1) * 192].astype(F32)
                    for j in range(4)
                ]
                dk[kb, rows, :] = jnp.concatenate(cuts, axis=1).astype(BF16)
            return carry

        lax.fori_loop(0, 8, repack, 0)

    def gather_step(r, carry):
        held = ((p2 + RING - r) % RING, (p2 + r) % RING)
        for h in range(2):
            for sub in range(h * 4, h * 4 + 4):
                for way in range(2):
                    ring_copy(way, r - 1, held[way], sub).wait_recv()
                    if h == way:
                        ring_copy(way, r, held[way], sub).start()
                    else:
                        @pl.when(r < 3)
                        def _():
                            ring_copy(way, r, held[way], sub).start()
            for way in range(2):
                project(held[way], h)
        return carry

    lax.fori_loop(1, 4, gather_step, 0)
    far = (p2 + 4) % RING
    for sub in range(4):
        for way in range(2):
            ring_copy(way, 3, far, way * 4 + sub).wait_recv()
    for way in range(2):
        project(far, way)

    remote(tabs.at[z_hi], tabs.at[1 - z_hi], t_send.at[0], t_recv.at[0], mirror).wait_recv()
    lane96 = lax.broadcasted_iota(jnp.int32, (128, 8), 1)
    for r in range(2):
        for xh in range(2):
            turned = jnp.transpose(tabs[r, 2 * c + xh])
            picked = jnp.sum(jnp.where(lane96 == e, turned, 0.0), axis=1, keepdims=True)
            scl[r, xh * 48:(xh + 1) * 48, :] = jnp.broadcast_to(picked[0:48], (48, 128))
        gate = acc[r, :, 0:256]
        up = acc[r, :, 256:512]
        hid[r] = (gate / (1.0 + jnp.exp(-gate)) * up).astype(BF16)
    everyone = tabs[0, 0]
    for k in range(1, 8):
        everyone = everyone + tabs[k // 4, k % 4]
    load_ref[...] = jnp.transpose(everyone)[48:50, :] / 48.0

    def own_part(q, h):
        kb, r = place(q, h)
        part = jnp.dot(hid[r], dk[kb], preferred_element_type=F32)
        return part * scl[r][:, 0:1]

    def sum_copy(way, s, sub):
        target = on_rings(p1, (p2 + (1 if way == 0 else 7)) % RING)
        return remote(
            sent.at[way, s, sub], came.at[way, s, sub],
            r_send.at[0], r_recv.at[way, s, sub], target,
        )

    def prepare(s, k, way):
        q = (p2 + (4 - s if way == 0 else 4 + s)) % RING
        ahead[way, k] = own_part(q, 1 - way if k == 0 else way)

    def pass_on(s, k, way, has_come):
        h = 1 - way if k == 0 else way
        for xh in range(2):
            sub = h * 2 + xh
            value = ahead[way, k, xh * 48:(xh + 1) * 48, :]
            if has_come:
                sum_copy(way, s - 1, sub).wait_recv()
                value = value + came[way, s - 1, sub].astype(F32)
            sent[way, s, sub] = value.astype(BF16)
            sum_copy(way, s, sub).start()

    for way in range(2):
        prepare(0, 1, way)
        pass_on(0, 1, way, False)
    for way in range(2):
        prepare(1, 0, way)
        pass_on(1, 0, way, False)
    for way in range(2):
        prepare(1, 1, way)
    for way in range(2):
        prepare(2, 0, way)
    for way in range(2):
        pass_on(1, 1, way, True)
        prepare(2, 1, way)

    def sum_step(s, carry):
        for way in range(2):
            pass_on(s, 0, way, True)
            prepare(s + 1, 0, way)
        for way in range(2):
            pass_on(s, 1, way, True)

            @pl.when(s < 3)
            def _():
                prepare(s + 1, 1, way)
        return carry

    lax.fori_loop(2, 4, sum_step, 0)

    scatter = lambda k: remote(
        own16.at[(p1 + k) % RING], direct.at[k], l_send.at[0], l_recv.at[k],
        on_rings((p1 + k) % RING, p2),
    )
    for h in range(2):
        halves = []
        for xh in range(2):
            sub = h * 2 + xh
            value = ahead[1 - h, 0, xh * 48:(xh + 1) * 48, :]
            for way in range(2):
                sum_copy(way, 3, sub).wait_recv()
                value = value + came[way, 3, sub].astype(F32)
            halves.append(value)
        for lo in range(4):
            both = jnp.concatenate([v[:, lo * 192:(lo + 1) * 192] for v in halves], axis=1)
            own32[h * 4 + lo] = both
            own16[h * 4 + lo] = both.astype(BF16)

    @pl.when(c == 0)
    def _():
        pl.semaphore_signal(pair_sem, inc=1, device_id=sibling, device_id_type=MESH)

    @pl.when(c == 1)
    def _():
        pl.semaphore_wait(pair_sem, 1)

    for k in (4, 3, 5, 2, 6, 1, 7):
        scatter(k).start()
    total = own32[p1]
    for k in (1, 7, 2, 6, 3, 5, 4):
        scatter(k).wait_recv()
        total = total + direct[k].astype(F32)
    for xt in range(2):
        for ct in range(2):
            last_out[xt, ct] = total[:, xt * 192 + ct * 96:xt * 192 + (ct + 1) * 96]

    def home(xt, ct):
        return remote(
            last_out.at[xt, ct], last_in.at[x], o_send.at[xt, ct], o_recv.at[x],
            device(2 * c + xt, y, z, ct),
        )

    for xt in range(2):
        for ct in range(2):
            @pl.when((2 * c + xt != x) | (c != ct))
            def _():
                home(xt, ct).start()

    @pl.when(half == c)
    def _():
        last_in[x] = last_out[x % 2, c]

    for d in (1, 2, 3):
        table(d).wait_send()
        remote(
            tok_ref, near.at[x % 2, c], x_send.at[d], x_recv.at[x % 2, c],
            device((x + d) % 4, y, z, half),
        ).wait_send()

    @pl.when(half != c)
    def _():
        remote(tok_ref, near.at[x % 2, c], x_send.at[0], x_recv.at[x % 2, c], sibling).wait_send()

    far_table.wait_send()
    down_copy.wait_send()
    for k in range(2):
        mine = wk.at[:, :, pl.ds(pl.multiple_of((2 * k + c) * 128, 128), 128)]
        pltpu.make_async_copy(mine, mine, w_sem.at[2 + k]).wait()

    for sem, kept in ((f_send, first), (l_send, own16), (a_send, blocks), (r_send, blocks)):
        gone = kept.at[pl.ds(0, 7)]
        pltpu.make_async_copy(gone, gone, sem.at[0]).wait()
    for xt in range(2):
        for ct in range(2):
            @pl.when((2 * c + xt != x) | (c != ct))
            def _():
                home(xt, ct).wait_send()

    for xs in range(4):
        @pl.when((xs != x) | (half != c))
        def _():
            remote(
                last_out.at[0, 0], last_in.at[xs], o_send.at[0, 0], o_recv.at[xs], sibling
            ).wait_recv()
    out_ref[...] = (last_in[0] + last_in[1] + last_in[2] + last_in[3]).astype(BF16)

def local(tokens, expert_ids, route_weight, gate_weight, up_weight, down_weight):
    vmem, dma = pltpu.VMEM, pltpu.SemaphoreType.DMA
    inside = pl.BlockSpec(memory_space=pltpu.VMEM)
    outside = pl.BlockSpec(memory_space=pltpu.HBM)
    return pl.pallas_call(
        kernel,
        name="layer",
        out_shape=(
            jax.ShapeDtypeStruct((48, 96), BF16),
            jax.ShapeDtypeStruct((2, 8), F32),
        ),
        in_specs=[outside] * 6,
        out_specs=(inside, inside),
        scratch_shapes=[
            vmem((48, 96), BF16),
            vmem((2, 48), jnp.int32),
            vmem((2, 48), jnp.int32),
            vmem((2, 2, 48, 96), BF16),
            vmem((2, 4, 8, 128), F32),
            vmem((8, 48, 384), BF16),
            vmem((8, 8, 48, 384), BF16),
            vmem((8, 768, 512), BF16),
            vmem((256, 6144), BF16),
            vmem((8, 256, 768), BF16),
            vmem((2, 96, 512), F32),
            vmem((2, 96, 256), BF16),
            vmem((2, 96, 128), F32),
            vmem((2, 2, 96, 768), F32),
            vmem((2, 4, 4, 48, 768), BF16),
            vmem((2, 4, 4, 48, 768), BF16),
            vmem((8, 48, 384), F32),
            vmem((8, 48, 384), BF16),
            vmem((8, 48, 384), BF16),
            vmem((2, 2, 48, 96), F32),
            vmem((4, 48, 96), F32),
            dma((3,)),
            dma((6,)),
            dma((3,)),
            dma((4,)),
            dma((2, 2)),
            dma((4,)),
            dma((4,)),
            dma((1,)),
            dma((8,)),
            dma((1,)),
            dma((2, 4, 8)),
            dma((1,)),
            dma((2, 4, 4)),
            dma((1,)),
            dma((8,)),
            dma((2, 2)),
            dma((4,)),
            pltpu.SemaphoreType.REGULAR,
        ],
        compiler_params=pltpu.CompilerParams(
            collective_id=0, has_side_effects=True, vmem_limit_bytes=48 * 1024 * 1024
        ),
    )(*[
        pltpu.with_memory_space_constraint(a, pltpu.HBM)
        for a in (tokens, expert_ids.T, route_weight.T, gate_weight, up_weight, down_weight)
    ])


def solution(mesh):
    placed = (
        P("expert", "tensor"),
        P("expert", None),
        P("expert", None),
        P("expert", None, "tensor"),
        P("expert", None, "tensor"),
        P("expert", "tensor", None),
    )
    return jax.shard_map(
        local, mesh=mesh, in_specs=placed, out_specs=(P("expert", "tensor"), P()), check_vma=False
    )
```

```python
import jax
import jax.numpy as jnp
from jax import lax
from jax.experimental import pallas as pl
from jax.experimental.pallas import tpu as pltpu
from jax.sharding import PartitionSpec as P

MESH = pl.DeviceIdType.MESH
F32 = jnp.float32
BF16 = jnp.bfloat16
RING = 8


def kernel(
    tok_hbm, ids_hbm, raw_hbm, gate_ref, up_ref, down_ref,
    out_ref, load_ref,
    tok_ref, ids_ref, raw_ref, near, tabs, first, blocks, wk, dn, dk, acc, hid, scl, ahead,
    sent, came, own32, own16, direct, last_out, last_in,
    in_sem, w_sem, d_sem, x_send, x_recv, t_send, t_recv, f_send, f_recv,
    a_send, a_recv, r_send, r_recv, l_send, l_recv, o_send, o_recv,
):
    e = lax.axis_index("expert")
    t = lax.axis_index("tensor")
    x, z_hi = e // 2, e % 2
    y, z_lo, c = t // 8, (t // 2) % 4, t % 2
    z = z_hi * 4 + z_lo
    half = x // 2
    role = (c + y + z) % 2
    p1 = z + role * (y - z)
    p2 = y + role * (z - y)

    def device(x_, y_, z_, c_):
        return (x_ * 2 + z_ // 4, (y_ * 4 + z_ % 4) * 2 + c_)

    def on_rings(a, b):
        y_, z_ = b + role * (a - b), a + role * (b - a)
        return device(x, y_, z_, (role + y_ + z_) % 2)

    def remote(src, dst, send, recv, target):
        return pltpu.make_async_remote_copy(
            src_ref=src, dst_ref=dst, send_sem=send, recv_sem=recv,
            device_id=target, device_id_type=MESH,
        )

    sibling = device(x, y, z, 1 - c)

    barrier = pltpu.get_barrier_semaphore()

    def greet(target):
        pl.semaphore_signal(barrier, inc=1, device_id=target, device_id_type=MESH)

    for k in (4, 3, 5, 2, 6, 1, 7):
        other = (x * 2 + c + k) % 8
        greet(on_rings((p1 + k) % RING, p2))
        if k in (1, 4, 7):
            greet(on_rings(p1, (p2 + k) % RING))
        greet(device(other // 2, y, z, other % 2))

    def weight_rows(i, path):
        kb, j = i // 4, i % 4
        straight = kb * 768 + j * 192
        across = ((kb % 2) * 4 + j) * 768 + (kb // 2) * 192
        return pl.ds(pl.multiple_of(straight + path * (across - straight), 64), 192)

    def weight_slot(i, k):
        return wk.at[i // 4, pl.ds(pl.multiple_of((i % 4) * 192, 64), 192), pl.ds(pl.multiple_of(k * 128, 128), 128)]

    def local_weights(i, carry):
        rows = weight_rows(i, role)
        pltpu.make_async_copy(gate_ref.at[0, rows, :], weight_slot(i, c), w_sem.at[0]).start()
        pltpu.make_async_copy(up_ref.at[0, rows, :], weight_slot(i, 2 + c), w_sem.at[1]).start()
        return carry

    tok_copy = pltpu.make_async_copy(tok_hbm, tok_ref, in_sem.at[0])
    ids_copy = pltpu.make_async_copy(ids_hbm, ids_ref, in_sem.at[1])
    raw_copy = pltpu.make_async_copy(raw_hbm, raw_ref, in_sem.at[2])
    tok_copy.start()
    ids_copy.start()
    raw_copy.start()
    own_down = dn.at[pl.ds(pl.multiple_of(c * 128, 128), 128), :]
    their_down = dn.at[pl.ds(pl.multiple_of((1 - c) * 128, 128), 128), :]
    pltpu.make_async_copy(down_ref.at[0], own_down, d_sem.at[0]).start()

    lax.fori_loop(0, 32, local_weights, 0)

    ids_copy.wait()
    raw_copy.wait()
    row = lax.broadcasted_iota(jnp.int32, (8, 48), 0)
    weights = raw_ref[...].astype(F32)
    share = weights / (weights[0:1, :] + weights[1:2, :])
    ids = ids_ref[...]
    zero = jnp.zeros((8, 48), F32)
    hit0 = ids[0:1, :] == row
    hit1 = ids[1:2, :] == row
    mix = jnp.where(hit0, share[0:1, :], zero) + jnp.where(hit1, share[1:2, :], zero)
    hits = jnp.where(hit0, 1.0, zero) + jnp.where(hit1, 1.0, zero)
    tabs[z_hi, x, :, 0:48] = mix
    tabs[z_hi, x, :, 48:128] = jnp.where(
        lax.broadcasted_iota(jnp.int32, (8, 80), 1) == 0,
        jnp.sum(hits, axis=1, keepdims=True), jnp.sum(mix, axis=1, keepdims=True),
    )

    tok_copy.wait()
    pl.semaphore_wait(barrier, 17)

    for d in (2, 1, 3):
        remote(
            tok_ref, near.at[x % 2, c], x_send.at[d], x_recv.at[x % 2, c],
            device((x + d) % 4, y, z, (half + y + z) % 2),
        ).start()

    @pl.when(half != role)
    def _():
        remote(tok_ref, near.at[x % 2, c], x_send.at[0], x_recv.at[x % 2, c], sibling).start()

    @pl.when(half == role)
    def _():
        near[x % 2, c] = tok_ref[...]

    table = lambda d: remote(
        tabs.at[z_hi, x], tabs.at[z_hi, x], t_send.at[d], t_recv.at[d],
        device((x + d) % 4, y, z, c),
    )
    for d in (1, 2, 3):
        table(d).start()

    def remote_weights(i, carry):
        rows = weight_rows(i, 1 - role)
        remote(gate_ref.at[0, rows, :], weight_slot(i, c), w_sem.at[2], w_sem.at[4], sibling).start()
        remote(up_ref.at[0, rows, :], weight_slot(i, 2 + c), w_sem.at[3], w_sem.at[5], sibling).start()
        return carry

    down_copy = remote(down_ref.at[0], own_down, d_sem.at[1], d_sem.at[2], sibling)
    down_copy.start()
    lax.fori_loop(0, 32, remote_weights, 0)

    for xh in range(2):
        for cs in range(2):
            @pl.when((2 * role + xh != x) | (c != cs))
            def _():
                remote(
                    tok_ref, near.at[xh, cs], x_send.at[0], x_recv.at[xh, cs], sibling
                ).wait_recv()

    pieces = [near[xh, cs].astype(F32) for xh in range(2) for cs in range(2)]
    first[p1] = jnp.concatenate(pieces, axis=1).astype(BF16)

    around = lambda k: remote(
        first.at[p1], first.at[p1], f_send.at[0], f_recv.at[k], on_rings((p1 + k) % RING, p2)
    )
    for k in (1, 7, 4, 3, 5, 2, 6):
        around(k).start()
    for d in (1, 2, 3):
        remote(
            tabs.at[z_hi, x], tabs.at[z_hi, (x + 4 - d) % 4], t_send.at[d], t_recv.at[d], sibling
        ).wait_recv()
    mirror = device(x, y, (z + 4) % 8, c)
    far_table = remote(tabs.at[z_hi], tabs.at[z_hi], t_send.at[0], t_recv.at[0], mirror)
    far_table.start()

    acc[...] = jnp.zeros_like(acc)

    pair = p1 // 2
    pairs = [pair, (pair + 1) % 4, (pair + 3) % 4, (pair + 2) % 4]

    def near_first(h, rank):
        same = (pair // 2 + h + 1) % 2
        return (pair % 2 + 1 - same + rank) % 2

    def piece(pr, xh):
        return (pr // 2) * 4 + xh * 2 + pr % 2

    pltpu.make_async_copy(down_ref.at[0], own_down, d_sem.at[0]).wait()
    pltpu.make_async_copy(down_ref.at[0], their_down, d_sem.at[2]).wait()

    @pl.when(role == 0)
    def _():
        for kb in range(8):
            dk[kb] = dn[:, kb * 768:(kb + 1) * 768]

    @pl.when(role == 1)
    def _():
        def repack(g, carry):
            rows = pl.ds(pl.multiple_of(g * 32, 32), 32)
            for kb in range(8):
                lo, hi = kb // 2, kb % 2
                cuts = [
                    dn[rows, (hi * 4 + j) * 768 + lo * 192:(hi * 4 + j) * 768 + (lo + 1) * 192].astype(F32)
                    for j in range(4)
                ]
                dk[kb, rows, :] = jnp.concatenate(cuts, axis=1).astype(BF16)
            return carry

        lax.fori_loop(0, 8, repack, 0)

    def ring_copy(way, step, b, sub):
        target = on_rings(p1, (p2 + (1 if way == 0 else 7)) % RING)
        return remote(
            blocks.at[b, sub], blocks.at[b, sub],
            a_send.at[0], a_recv.at[way, step, sub], target,
        )

    def first_come(source):
        k = (p1 + RING - source) % RING
        remote(first.at[p1], first.at[source], f_send.at[0], f_recv.at[k], sibling).wait_recv()

    for j in range(4):
        if j == 0:
            first_come(p1 + 1 - 2 * (p1 % 2))
        else:
            first_come(pairs[j] * 2)
            first_come(pairs[j] * 2 + 1)
        for xh in range(2):
            sub = piece(pairs[j], xh)
            parts = [
                first[pairs[j] * 2 + lo][:, xh * 192:(xh + 1) * 192].astype(F32) for lo in range(2)
            ]
            blocks[p2, sub] = jnp.concatenate(parts, axis=1).astype(BF16)
            ring_copy(0, 0, p2, sub).start()
            ring_copy(1, 0, p2, sub).start()

    def place(b, h):
        across = (b % 4) * 2 + h
        return b + role * (across - b), h + role * (b // 4 - h)

    def project(b, h):
        kb, r = place(b, h)
        part = blocks[b, pl.ds(4 * h, 4)]
        rows = jnp.concatenate(
            [jnp.concatenate([part[2 * xh], part[2 * xh + 1]], axis=1) for xh in range(2)], axis=0
        )
        acc[r] += jnp.dot(rows, wk[kb], preferred_element_type=F32)

    def weights_here():
        for k in range(2):
            mine = wk.at[:, :, pl.ds(pl.multiple_of((2 * k + c) * 128, 128), 128)]
            theirs = wk.at[:, :, pl.ds(pl.multiple_of((2 * k + 1 - c) * 128, 128), 128)]
            pltpu.make_async_copy(mine, mine, w_sem.at[k]).wait()
            pltpu.make_async_copy(theirs, theirs, w_sem.at[4 + k]).wait()

    def gather_step(r, carry):
        held = ((p2 + RING - r) % RING, (p2 + r) % RING)
        before = ((p2 + RING + 1 - r) % RING, (p2 + r - 1) % RING)
        for j in range(4):
            h = pairs[j] // 2
            for xh in range(2):
                sub = piece(pairs[j], xh)
                for way in range(2):
                    ring_copy(way, r - 1, held[way], sub).wait_recv()

                    @pl.when((r < 3) | (h == way))
                    def _():
                        ring_copy(way, r, held[way], sub).start()

                if xh == 0 and j == 0:
                    pl.when(r == 1)(weights_here)
                if xh == 0 and j % 2 == 0:
                    project(before[0], j // 2)
                elif xh == 0:
                    @pl.when(r > 1)
                    def _():
                        project(before[1], j // 2)
        return carry

    lax.fori_loop(1, 4, gather_step, 0)
    far = (p2 + 4) % RING
    for rank in range(2):
        for xh in range(2):
            for way in range(2):
                sub = way * 4 + xh * 2 + near_first(way, rank)
                ring_copy(way, 3, far, sub).wait_recv()
            project((p2 + (5 if xh == 0 else 3)) % RING, rank)
    for way in range(2):
        project(far, way)

    remote(tabs.at[z_hi], tabs.at[1 - z_hi], t_send.at[0], t_recv.at[0], mirror).wait_recv()
    lane96 = lax.broadcasted_iota(jnp.int32, (128, 8), 1)
    for r in range(2):
        for xh in range(2):
            turned = jnp.transpose(tabs[r, 2 * role + xh])
            picked = jnp.sum(jnp.where(lane96 == e, turned, 0.0), axis=1, keepdims=True)
            scl[r, xh * 48:(xh + 1) * 48, :] = jnp.broadcast_to(picked[0:48], (48, 128))
        gate = acc[r, :, 0:256]
        up = acc[r, :, 256:512]
        hid[r] = (gate / (1.0 + jnp.exp(-gate)) * up).astype(BF16)
    everyone = tabs[0, 0]
    for k in range(1, 8):
        everyone = everyone + tabs[k // 4, k % 4]
    load_ref[...] = jnp.transpose(everyone)[48:50, :] / 48.0

    def own_part(q, h):
        kb, r = place(q, h)
        part = jnp.dot(hid[r], dk[kb], preferred_element_type=F32)
        return part * scl[r][:, 0:1]

    def sum_copy(way, s, sub):
        target = on_rings(p1, (p2 + (1 if way == 0 else 7)) % RING)
        return remote(
            sent.at[way, s, sub], came.at[way, s, sub],
            r_send.at[0], r_recv.at[way, s, sub], target,
        )

    def prepare(s, k, way):
        q = (p2 + (4 - s if way == 0 else 4 + s)) % RING
        part = own_part(q, 1 - way if k == 0 else way)
        for xh in range(2):
            for lh in range(2):
                ahead[way, k, xh, lh] = part[xh * 48:(xh + 1) * 48, lh * 384:(lh + 1) * 384]

    def pass_on(s, k, has_come, following=None):
        for i in range(4):
            xh = i % 2
            for way in range(2):
                h = 1 - way if k == 0 else way
                lh = near_first(h, 1 - i // 2)
                sub = h * 4 + xh * 2 + lh
                value = ahead[way, k, xh, lh]
                if has_come:
                    sum_copy(way, s - 1, sub).wait_recv()
                    value = value + came[way, s - 1, sub].astype(F32)
                sent[way, s, sub] = value.astype(BF16)
                sum_copy(way, s, sub).start()
            if following is not None and i % 2 == 0:
                prepare(*following, i // 2)

    for way in range(2):
        prepare(0, 1, way)
    pass_on(0, 1, False, (1, 0))
    pass_on(1, 0, False)
    for way in range(2):
        prepare(1, 1, way)
    pass_on(1, 1, True, (2, 0))

    def sum_step(s, carry):
        pass_on(s, 0, True, (s, 1))
        pass_on(s, 1, True, (s + 1, 0))
        return carry

    lax.fori_loop(2, 4, sum_step, 0)

    def scatter(target):
        k = (target + RING - p1) % RING
        return remote(
            own16.at[target], direct.at[k], l_send.at[0], l_recv.at[k], on_rings(target, p2)
        )

    def scatter_pair(pr):
        for lo in range(2):
            target = pr * 2 + lo

            @pl.when(target != p1)
            def _():
                scatter(target).start()

    for rank in (1, 0):
        for h in range(2):
            lh = near_first(h, rank)
            halves = []
            for xh in range(2):
                sub = h * 4 + xh * 2 + lh
                value = ahead[1 - h, 0, xh, lh]
                for way in (1 - h, h):
                    sum_copy(way, 3, sub).wait_recv()
                    value = value + came[way, 3, sub].astype(F32)
                halves.append(value)
            for lo in range(2):
                both = jnp.concatenate([v[:, lo * 192:(lo + 1) * 192] for v in halves], axis=1)
                own32[h * 4 + lh * 2 + lo] = both
                own16[h * 4 + lh * 2 + lo] = both.astype(BF16)

            scatter_pair(h * 2 + lh)

    for d in (1, 2, 3):
        table(d).wait_send()
        remote(
            tok_ref, near.at[x % 2, c], x_send.at[d], x_recv.at[x % 2, c],
            device((x + d) % 4, y, z, (half + y + z) % 2),
        ).wait_send()

    @pl.when(half != role)
    def _():
        remote(tok_ref, near.at[x % 2, c], x_send.at[0], x_recv.at[x % 2, c], sibling).wait_send()

    far_table.wait_send()
    down_copy.wait_send()
    for k in range(2):
        mine = wk.at[:, :, pl.ds(pl.multiple_of((2 * k + c) * 128, 128), 128)]
        pltpu.make_async_copy(mine, mine, w_sem.at[2 + k]).wait()

    for sem, kept in ((f_send, first), (a_send, blocks), (r_send, blocks)):
        gone = kept.at[pl.ds(0, 7)]
        pltpu.make_async_copy(gone, gone, sem.at[0]).wait()
    total = own32[p1]
    for k in (1, 7, 2, 6, 3, 5, 4):
        remote(own16.at[0], direct.at[k], l_send.at[0], l_recv.at[k], sibling).wait_recv()
        total = total + direct[k].astype(F32)
    for xt in range(2):
        for ct in range(2):
            last_out[xt, ct] = total[:, xt * 192 + ct * 96:xt * 192 + (ct + 1) * 96]

    def home(xt, ct):
        return remote(
            last_out.at[xt, ct], last_in.at[x], o_send.at[xt, ct], o_recv.at[x],
            device(2 * role + xt, y, z, ct),
        )

    for xt in range(2):
        for ct in range(2):
            @pl.when((2 * role + xt != x) | (c != ct))
            def _():
                home(xt, ct).start()

    @pl.when(half == role)
    def _():
        last_in[x] = last_out[x % 2, c]

    for xs in range(4):
        @pl.when((xs != x) | (half != role))
        def _():
            remote(
                last_out.at[0, 0], last_in.at[xs], o_send.at[0, 0], o_recv.at[xs], sibling
            ).wait_recv()
    out_ref[...] = (last_in[0] + last_in[1] + last_in[2] + last_in[3]).astype(BF16)
    for xt in range(2):
        for ct in range(2):
            @pl.when((2 * role + xt != x) | (c != ct))
            def _():
                home(xt, ct).wait_send()
    gone = own16.at[pl.ds(0, 7)]
    pltpu.make_async_copy(gone, gone, l_send.at[0]).wait()


def local(tokens, expert_ids, route_weight, gate_weight, up_weight, down_weight):
    vmem, dma = pltpu.VMEM, pltpu.SemaphoreType.DMA
    inside = pl.BlockSpec(memory_space=pltpu.VMEM)
    outside = pl.BlockSpec(memory_space=pltpu.HBM)
    return pl.pallas_call(
        kernel,
        name="layer",
        out_shape=(
            jax.ShapeDtypeStruct((48, 96), BF16),
            jax.ShapeDtypeStruct((2, 8), F32),
        ),
        in_specs=[outside] * 6,
        out_specs=(inside, inside),
        scratch_shapes=[
            vmem((48, 96), BF16),
            vmem((2, 48), jnp.int32),
            vmem((2, 48), jnp.int32),
            vmem((2, 2, 48, 96), BF16),
            vmem((2, 4, 8, 128), F32),
            vmem((8, 48, 384), BF16),
            vmem((8, 8, 48, 384), BF16),
            vmem((8, 768, 512), BF16),
            vmem((256, 6144), BF16),
            vmem((8, 256, 768), BF16),
            vmem((2, 96, 512), F32),
            vmem((2, 96, 256), BF16),
            vmem((2, 96, 128), F32),
            vmem((2, 2, 2, 2, 48, 384), F32),
            vmem((2, 4, 8, 48, 384), BF16),
            vmem((2, 4, 8, 48, 384), BF16),
            vmem((8, 48, 384), F32),
            vmem((8, 48, 384), BF16),
            vmem((8, 48, 384), BF16),
            vmem((2, 2, 48, 96), F32),
            vmem((4, 48, 96), F32),
            dma((3,)),
            dma((6,)),
            dma((3,)),
            dma((4,)),
            dma((2, 2)),
            dma((4,)),
            dma((4,)),
            dma((1,)),
            dma((8,)),
            dma((1,)),
            dma((2, 4, 8)),
            dma((1,)),
            dma((2, 4, 8)),
            dma((1,)),
            dma((8,)),
            dma((2, 2)),
            dma((4,)),
        ],
        compiler_params=pltpu.CompilerParams(
            collective_id=0, has_side_effects=True, vmem_limit_bytes=48 * 1024 * 1024
        ),
    )(*[
        pltpu.with_memory_space_constraint(a, pltpu.HBM)
        for a in (tokens, expert_ids.T, route_weight.T, gate_weight, up_weight, down_weight)
    ])


def solution(mesh):
    placed = (
        P("expert", "tensor"),
        P("expert", None),
        P("expert", None),
        P("expert", None, "tensor"),
        P("expert", None, "tensor"),
        P("expert", "tensor", None),
    )
    return jax.shard_map(
        local, mesh=mesh, in_specs=placed, out_specs=(P("expert", "tensor"), P()), check_vma=False
    )
```

```python
import jax
import jax.numpy as jnp
from jax import lax
from jax.experimental import pallas as pl
from jax.experimental.pallas import tpu as pltpu
from jax.sharding import PartitionSpec as P

MESH = pl.DeviceIdType.MESH
F32 = jnp.float32
BF16 = jnp.bfloat16
RING = 8


def kernel(
    tok_hbm, ids_hbm, raw_hbm, gate_ref, up_ref, down_ref,
    out_ref, load_ref,
    tok_ref, ids_ref, raw_ref, near, tabs, first, blocks, wk, dn, dk, acc, hid, scl, ahead,
    sent, came, own32, own16, direct, last_out, last_in,
    in_sem, w_sem, d_sem, x_send, x_recv, t_send, t_recv, f_send, f_recv,
    a_send, a_recv, r_send, r_recv, l_send, l_recv, o_send, o_recv,
):
    e = lax.axis_index("expert")
    t = lax.axis_index("tensor")
    x, z_hi = e // 2, e % 2
    y, z_lo, c = t // 8, (t // 2) % 4, t % 2
    z = z_hi * 4 + z_lo
    half = x // 2
    role = (c + y + z) % 2
    p1 = z + role * (y - z)
    p2 = y + role * (z - y)

    def device(x_, y_, z_, c_):
        return (x_ * 2 + z_ // 4, (y_ * 4 + z_ % 4) * 2 + c_)

    def on_rings(a, b):
        y_, z_ = b + role * (a - b), a + role * (b - a)
        return device(x, y_, z_, (role + y_ + z_) % 2)

    def remote(src, dst, send, recv, target):
        return pltpu.make_async_remote_copy(
            src_ref=src, dst_ref=dst, send_sem=send, recv_sem=recv,
            device_id=target, device_id_type=MESH,
        )

    sibling = device(x, y, z, 1 - c)

    barrier = pltpu.get_barrier_semaphore()

    def greet(target):
        pl.semaphore_signal(barrier, inc=1, device_id=target, device_id_type=MESH)

    for k in (4, 3, 5, 2, 6, 1, 7):
        other = (x * 2 + c + k) % 8
        greet(on_rings((p1 + k) % RING, p2))
        if k in (1, 4, 7):
            greet(on_rings(p1, (p2 + k) % RING))
        greet(device(other // 2, y, z, other % 2))

    def weight_rows(i, path):
        kb, j = i // 4, i % 4
        straight = kb * 768 + j * 192
        across = ((kb % 2) * 4 + j) * 768 + (kb // 2) * 192
        return pl.ds(pl.multiple_of(straight + path * (across - straight), 64), 192)

    def weight_slot(i, k):
        return wk.at[i // 4, pl.ds(pl.multiple_of((i % 4) * 192, 64), 192), pl.ds(pl.multiple_of(k * 128, 128), 128)]

    def local_weights(i, carry):
        rows = weight_rows(i, role)
        pltpu.make_async_copy(gate_ref.at[0, rows, :], weight_slot(i, c), w_sem.at[0]).start()
        pltpu.make_async_copy(up_ref.at[0, rows, :], weight_slot(i, 2 + c), w_sem.at[1]).start()
        return carry

    tok_copy = pltpu.make_async_copy(tok_hbm, tok_ref, in_sem.at[0])
    ids_copy = pltpu.make_async_copy(ids_hbm, ids_ref, in_sem.at[1])
    raw_copy = pltpu.make_async_copy(raw_hbm, raw_ref, in_sem.at[2])
    tok_copy.start()
    ids_copy.start()
    raw_copy.start()
    own_down = dn.at[pl.ds(pl.multiple_of(c * 128, 128), 128), :]
    their_down = dn.at[pl.ds(pl.multiple_of((1 - c) * 128, 128), 128), :]
    pltpu.make_async_copy(down_ref.at[0], own_down, d_sem.at[0]).start()

    lax.fori_loop(0, 32, local_weights, 0)

    ids_copy.wait()
    raw_copy.wait()
    row = lax.broadcasted_iota(jnp.int32, (8, 48), 0)
    weights = raw_ref[...].astype(F32)
    share = weights / (weights[0:1, :] + weights[1:2, :])
    ids = ids_ref[...]
    zero = jnp.zeros((8, 48), F32)
    hit0 = ids[0:1, :] == row
    hit1 = ids[1:2, :] == row
    mix = jnp.where(hit0, share[0:1, :], zero) + jnp.where(hit1, share[1:2, :], zero)
    hits = jnp.where(hit0, 1.0, zero) + jnp.where(hit1, 1.0, zero)
    tabs[z_hi, x, :, 0:48] = mix
    tabs[z_hi, x, :, 48:128] = jnp.where(
        lax.broadcasted_iota(jnp.int32, (8, 80), 1) == 0,
        jnp.sum(hits, axis=1, keepdims=True), jnp.sum(mix, axis=1, keepdims=True),
    )

    tok_copy.wait()
    pl.semaphore_wait(barrier, 17)

    for d in (2, 1, 3):
        remote(
            tok_ref, near.at[x % 2, c], x_send.at[d], x_recv.at[x % 2, c],
            device((x + d) % 4, y, z, (half + y + z) % 2),
        ).start()

    @pl.when(half != role)
    def _():
        remote(tok_ref, near.at[x % 2, c], x_send.at[0], x_recv.at[x % 2, c], sibling).start()

    @pl.when(half == role)
    def _():
        near[x % 2, c] = tok_ref[...]

    table = lambda d: remote(
        tabs.at[z_hi, x], tabs.at[z_hi, x], t_send.at[d], t_recv.at[d],
        device((x + d) % 4, y, z, c),
    )
    for d in (1, 2, 3):
        table(d).start()

    def remote_weights(i, carry):
        rows = weight_rows(i, 1 - role)
        remote(gate_ref.at[0, rows, :], weight_slot(i, c), w_sem.at[2], w_sem.at[4], sibling).start()
        remote(up_ref.at[0, rows, :], weight_slot(i, 2 + c), w_sem.at[3], w_sem.at[5], sibling).start()
        return carry

    down_copy = remote(down_ref.at[0], own_down, d_sem.at[1], d_sem.at[2], sibling)
    down_copy.start()
    lax.fori_loop(0, 32, remote_weights, 0)

    for xh in range(2):
        for cs in range(2):
            @pl.when((2 * role + xh != x) | (c != cs))
            def _():
                remote(
                    tok_ref, near.at[xh, cs], x_send.at[0], x_recv.at[xh, cs], sibling
                ).wait_recv()

    pieces = [near[xh, cs].astype(F32) for xh in range(2) for cs in range(2)]
    first[p1] = jnp.concatenate(pieces, axis=1).astype(BF16)

    around = lambda k: remote(
        first.at[p1], first.at[p1], f_send.at[0], f_recv.at[k], on_rings((p1 + k) % RING, p2)
    )
    for k in (4, 3, 5, 2, 6, 1, 7):
        around(k).start()
    for d in (1, 2, 3):
        remote(
            tabs.at[z_hi, x], tabs.at[z_hi, (x + 4 - d) % 4], t_send.at[d], t_recv.at[d], sibling
        ).wait_recv()
    mirror = device(x, y, (z + 4) % 8, c)
    far_table = remote(tabs.at[z_hi], tabs.at[z_hi], t_send.at[0], t_recv.at[0], mirror)
    far_table.start()

    acc[...] = jnp.zeros_like(acc)

    pair = p1 // 2
    pairs = [pair, (pair + 1) % 4, (pair + 3) % 4, (pair + 2) % 4]

    def near_first(h, rank):
        same = (pair // 2 + h + 1) % 2
        return (pair % 2 + 1 - same + rank) % 2

    def piece(pr, xh):
        return (pr // 2) * 4 + xh * 2 + pr % 2

    pltpu.make_async_copy(down_ref.at[0], own_down, d_sem.at[0]).wait()
    pltpu.make_async_copy(down_ref.at[0], their_down, d_sem.at[2]).wait()

    @pl.when(role == 0)
    def _():
        for kb in range(8):
            dk[kb] = dn[:, kb * 768:(kb + 1) * 768]

    @pl.when(role == 1)
    def _():
        def repack(g, carry):
            rows = pl.ds(pl.multiple_of(g * 32, 32), 32)
            for kb in range(8):
                lo, hi = kb // 2, kb % 2
                cuts = [
                    dn[rows, (hi * 4 + j) * 768 + lo * 192:(hi * 4 + j) * 768 + (lo + 1) * 192].astype(F32)
                    for j in range(4)
                ]
                dk[kb, rows, :] = jnp.concatenate(cuts, axis=1).astype(BF16)
            return carry

        lax.fori_loop(0, 8, repack, 0)

    def ring_copy(way, step, b, sub):
        target = on_rings(p1, (p2 + (1 if way == 0 else 7)) % RING)
        return remote(
            blocks.at[b, sub], blocks.at[b, sub],
            a_send.at[0], a_recv.at[way, step * 8 + sub - step // 3 * way * 4], target,
        )

    def first_come(source):
        k = (p1 + RING - source) % RING
        remote(first.at[p1], first.at[source], f_send.at[0], f_recv.at[k], sibling).wait_recv()

    for j in range(4):
        if j == 0:
            first_come(p1 + 1 - 2 * (p1 % 2))
        else:
            first_come(pairs[j] * 2)
            first_come(pairs[j] * 2 + 1)
        for xh in range(2):
            sub = piece(pairs[j], xh)
            parts = [
                first[pairs[j] * 2 + lo][:, xh * 192:(xh + 1) * 192].astype(F32) for lo in range(2)
            ]
            blocks[p2, sub] = jnp.concatenate(parts, axis=1).astype(BF16)
            ring_copy(0, 0, p2, sub).start()
            ring_copy(1, 0, p2, sub).start()

    def place(b, h):
        across = (b % 4) * 2 + h
        return b + role * (across - b), h + role * (b // 4 - h)

    def project(b, h):
        kb, r = place(b, h)
        part = blocks[b, pl.ds(4 * h, 4)]
        rows = jnp.concatenate(
            [jnp.concatenate([part[2 * xh], part[2 * xh + 1]], axis=1) for xh in range(2)], axis=0
        )
        acc[r] += jnp.dot(rows, wk[kb], preferred_element_type=F32)

    def weights_here():
        for k in range(2):
            mine = wk.at[:, :, pl.ds(pl.multiple_of((2 * k + c) * 128, 128), 128)]
            theirs = wk.at[:, :, pl.ds(pl.multiple_of((2 * k + 1 - c) * 128, 128), 128)]
            pltpu.make_async_copy(mine, mine, w_sem.at[k]).wait()
            pltpu.make_async_copy(theirs, theirs, w_sem.at[4 + k]).wait()

    def gather_step(r, carry):
        held = ((p2 + RING - r) % RING, (p2 + r) % RING)
        before = ((p2 + RING + 1 - r) % RING, (p2 + r - 1) % RING)
        for j in range(4):
            h = pairs[j] // 2
            for xh in range(2):
                sub = piece(pairs[j], xh)
                for way in range(2):
                    ring_copy(way, r - 1, held[way], sub).wait_recv()

                    @pl.when((r < 3) | (h == way))
                    def _():
                        ring_copy(way, r, held[way], sub).start()

                if xh == 0 and j == 0:
                    pl.when(r == 1)(weights_here)
                if xh == 0 and j % 2 == 0:
                    project(before[0], j // 2)
                elif xh == 0:
                    @pl.when(r > 1)
                    def _():
                        project(before[1], j // 2)
        return carry

    lax.fori_loop(1, 4, gather_step, 0)
    remote(tabs.at[z_hi], tabs.at[1 - z_hi], t_send.at[0], t_recv.at[0], mirror).wait_recv()
    lane96 = lax.broadcasted_iota(jnp.int32, (128, 8), 1)
    for r in range(2):
        for xh in range(2):
            turned = jnp.transpose(tabs[r, 2 * role + xh])
            picked = jnp.sum(jnp.where(lane96 == e, turned, 0.0), axis=1, keepdims=True)
            scl[r, xh * 48:(xh + 1) * 48, :] = jnp.broadcast_to(picked[0:48], (48, 128))
    everyone = tabs[0, 0]
    for k in range(1, 8):
        everyone = everyone + tabs[k // 4, k % 4]
    load_ref[...] = jnp.transpose(everyone)[48:50, :] / 48.0

    far = (p2 + 4) % RING
    for rank in range(2):
        for xh in range(2):
            for way in range(2):
                sub = way * 4 + xh * 2 + near_first(way, rank)
                ring_copy(way, 3, far, sub).wait_recv()
            project((p2 + (5 if xh == 0 else 3)) % RING, rank)
    for way in range(2):
        project(far, way)

    for r in range(2):
        gate = acc[r, :, 0:256]
        up = acc[r, :, 256:512]
        hid[r] = (gate / (1.0 + jnp.exp(-gate)) * up).astype(BF16)

    def own_part(q, h):
        kb, r = place(q, h)
        part = jnp.dot(hid[r], dk[kb], preferred_element_type=F32)
        return part * scl[r][:, 0:1]

    def sum_copy(way, s, sub):
        target = on_rings(p1, (p2 + (1 if way == 0 else 7)) % RING)
        return remote(
            sent.at[way, s, sub], came.at[way, s, sub],
            r_send.at[0], r_recv.at[way, (s * 8 + sub - 4) if s is not None and not isinstance(s, int) else (sub - way * 4 if s == 0 else s * 8 + sub - 4)], target,
        )

    def prepare(s, k, way):
        q = (p2 + (4 - s if way == 0 else 4 + s)) % RING
        part = own_part(q, 1 - way if k == 0 else way)
        for xh in range(2):
            for lh in range(2):
                ahead[way, k, xh, lh] = part[xh * 48:(xh + 1) * 48, lh * 384:(lh + 1) * 384]

    def pass_on(s, k, has_come, following=None):
        for i in range(4):
            xh = i % 2
            for way in range(2):
                h = 1 - way if k == 0 else way
                lh = near_first(h, 1 - i // 2)
                sub = h * 4 + xh * 2 + lh
                value = ahead[way, k, xh, lh]
                if has_come:
                    sum_copy(way, s - 1, sub).wait_recv()
                    value = value + came[way, s - 1, sub].astype(F32)
                sent[way, s, sub] = value.astype(BF16)
                sum_copy(way, s, sub).start()
            if following is not None and i % 2 == 0:
                prepare(*following, i // 2)

    for way in range(2):
        prepare(0, 1, way)
    pass_on(0, 1, False, (1, 0))
    pass_on(1, 0, False)
    for way in range(2):
        prepare(1, 1, way)
    pass_on(1, 1, True, (2, 0))

    def sum_step(s, carry):
        pass_on(s, 0, True, (s, 1))
        pass_on(s, 1, True, (s + 1, 0))
        return carry

    lax.fori_loop(2, 4, sum_step, 0)

    def scatter(target):
        k = (target + RING - p1) % RING
        return remote(
            own16.at[target], direct.at[k], l_send.at[0], l_recv.at[k], on_rings(target, p2)
        )

    def scatter_pair(pr):
        for lo in range(2):
            target = pr * 2 + lo

            @pl.when(target != p1)
            def _():
                scatter(target).start()

    for rank in (1, 0):
        for h in range(2):
            lh = near_first(h, rank)
            halves = []
            for xh in range(2):
                sub = h * 4 + xh * 2 + lh
                value = ahead[1 - h, 0, xh, lh]
                for way in (1 - h, h):
                    sum_copy(way, 3, sub).wait_recv()
                    value = value + came[way, 3, sub].astype(F32)
                halves.append(value)
            for lo in range(2):
                both = jnp.concatenate([v[:, lo * 192:(lo + 1) * 192] for v in halves], axis=1)
                own32[h * 4 + lh * 2 + lo] = both
                own16[h * 4 + lh * 2 + lo] = both.astype(BF16)

            scatter_pair(h * 2 + lh)

    for d in (1, 2, 3):
        table(d).wait_send()
        remote(
            tok_ref, near.at[x % 2, c], x_send.at[d], x_recv.at[x % 2, c],
            device((x + d) % 4, y, z, (half + y + z) % 2),
        ).wait_send()

    @pl.when(half != role)
    def _():
        remote(tok_ref, near.at[x % 2, c], x_send.at[0], x_recv.at[x % 2, c], sibling).wait_send()

    far_table.wait_send()
    down_copy.wait_send()
    for k in range(2):
        mine = wk.at[:, :, pl.ds(pl.multiple_of((2 * k + c) * 128, 128), 128)]
        pltpu.make_async_copy(mine, mine, w_sem.at[2 + k]).wait()

    for sem, kept in ((f_send, first), (a_send, blocks), (r_send, blocks)):
        gone = kept.at[pl.ds(0, 7)]
        pltpu.make_async_copy(gone, gone, sem.at[0]).wait()
    total = own32[p1]
    for k in (1, 7, 2, 6, 3, 5, 4):
        remote(own16.at[0], direct.at[k], l_send.at[0], l_recv.at[k], sibling).wait_recv()
        total = total + direct[k].astype(F32)
    for xt in range(2):
        for ct in range(2):
            last_out[xt, ct] = total[:, xt * 192 + ct * 96:xt * 192 + (ct + 1) * 96]

    def home(xt, ct):
        return remote(
            last_out.at[xt, ct], last_in.at[x], o_send.at[xt, ct], o_recv.at[x],
            device(2 * role + xt, y, z, ct),
        )

    for xt in range(2):
        for ct in range(2):
            @pl.when((2 * role + xt != x) | (c != ct))
            def _():
                home(xt, ct).start()

    @pl.when(half == role)
    def _():
        last_in[x] = last_out[x % 2, c]

    for xs in range(4):
        @pl.when((xs != x) | (half != role))
        def _():
            remote(
                last_out.at[0, 0], last_in.at[xs], o_send.at[0, 0], o_recv.at[xs], sibling
            ).wait_recv()
    out_ref[...] = (last_in[0] + last_in[1] + last_in[2] + last_in[3]).astype(BF16)
    for xt in range(2):
        for ct in range(2):
            @pl.when((2 * role + xt != x) | (c != ct))
            def _():
                home(xt, ct).wait_send()
    gone = own16.at[pl.ds(0, 7)]
    pltpu.make_async_copy(gone, gone, l_send.at[0]).wait()


def hand_out(mixed_ref, load_ref, mixed_out, load_out, sem):
    copies = [
        pltpu.make_async_copy(mixed_ref, mixed_out, sem.at[0]),
        pltpu.make_async_copy(load_ref, load_out, sem.at[1]),
    ]
    for copy in copies:
        copy.start()
    for copy in copies:
        copy.wait()


def local(tokens, expert_ids, route_weight, gate_weight, up_weight, down_weight):
    vmem, dma = pltpu.VMEM, pltpu.SemaphoreType.DMA
    inside = pl.BlockSpec(memory_space=pltpu.VMEM)
    outside = pl.BlockSpec(memory_space=pltpu.HBM)
    shapes = (jax.ShapeDtypeStruct((48, 96), BF16), jax.ShapeDtypeStruct((2, 8), F32))
    result = pl.pallas_call(
        kernel,
        name="layer",
        out_shape=(
            jax.ShapeDtypeStruct((48, 96), BF16),
            jax.ShapeDtypeStruct((2, 8), F32),
        ),
        in_specs=[outside] * 6,
        out_specs=(inside, inside),
        scratch_shapes=[
            vmem((48, 96), BF16),
            vmem((2, 48), jnp.int32),
            vmem((2, 48), jnp.int32),
            vmem((2, 2, 48, 96), BF16),
            vmem((2, 4, 8, 128), F32),
            vmem((8, 48, 384), BF16),
            vmem((8, 8, 48, 384), BF16),
            vmem((8, 768, 512), BF16),
            vmem((256, 6144), BF16),
            vmem((8, 256, 768), BF16),
            vmem((2, 96, 512), F32),
            vmem((2, 96, 256), BF16),
            vmem((2, 96, 128), F32),
            vmem((2, 2, 2, 2, 48, 384), F32),
            vmem((2, 4, 8, 48, 384), BF16),
            vmem((2, 4, 8, 48, 384), BF16),
            vmem((8, 48, 384), F32),
            vmem((8, 48, 384), BF16),
            vmem((8, 48, 384), BF16),
            vmem((2, 2, 48, 96), F32),
            vmem((4, 48, 96), F32),
            dma((3,)),
            dma((6,)),
            dma((3,)),
            dma((4,)),
            dma((2, 2)),
            dma((4,)),
            dma((4,)),
            dma((1,)),
            dma((8,)),
            dma((1,)),
            dma((2, 28)),
            dma((1,)),
            dma((2, 28)),
            dma((1,)),
            dma((8,)),
            dma((2, 2)),
            dma((4,)),
        ],
        compiler_params=pltpu.CompilerParams(
            collective_id=0, has_side_effects=True, vmem_limit_bytes=48 * 1024 * 1024
        ),
    )(*[
        pltpu.with_memory_space_constraint(a, pltpu.HBM)
        for a in (tokens, expert_ids.T, route_weight.T, gate_weight, up_weight, down_weight)
    ])
    return pl.pallas_call(
        hand_out,
        name="hand_out",
        out_shape=shapes,
        in_specs=[inside] * 2,
        out_specs=(outside, outside),
        scratch_shapes=[dma((2,))],
        compiler_params=pltpu.CompilerParams(vmem_limit_bytes=1024 * 1024),
    )(*result)


def solution(mesh):
    placed = (
        P("expert", "tensor"),
        P("expert", None),
        P("expert", None),
        P("expert", None, "tensor"),
        P("expert", None, "tensor"),
        P("expert", "tensor", None),
    )
    return jax.shard_map(
        local, mesh=mesh, in_specs=placed, out_specs=(P("expert", "tensor"), P()), check_vma=False
    )
```

```python
import jax
import jax.numpy as jnp
from jax import lax
from jax.experimental import pallas as pl
from jax.experimental.pallas import tpu as pltpu
from jax.sharding import PartitionSpec as P

MESH = pl.DeviceIdType.MESH
F32 = jnp.float32
BF16 = jnp.bfloat16
RING = 8


def kernel(
    tok_hbm, ids_hbm, raw_hbm, gate_ref, up_ref, down_ref,
    out_ref, load_ref,
    tok_ref, ids_ref, raw_ref, near, tabs, first, blocks, wk, dn, dk, acc, hid, scl, ahead,
    sent, came, own32, own16, direct, last_out, last_in,
    in_sem, w_sem, d_sem, x_send, x_recv, t_send, t_recv, f_send, f_recv,
    a_send, a_recv, r_send, r_recv, l_send, l_recv, o_send, o_recv,
):
    e = lax.axis_index("expert")
    t = lax.axis_index("tensor")
    x, z_hi = e // 2, e % 2
    y, z_lo, c = t // 8, (t // 2) % 4, t % 2
    z = z_hi * 4 + z_lo
    half = x // 2
    role = (c + y + z) % 2
    p1 = z + role * (y - z)
    p2 = y + role * (z - y)

    def device(x_, y_, z_, c_):
        return (x_ * 2 + z_ // 4, (y_ * 4 + z_ % 4) * 2 + c_)

    def on_rings(a, b):
        y_, z_ = b + role * (a - b), a + role * (b - a)
        return device(x, y_, z_, (role + y_ + z_) % 2)

    def remote(src, dst, send, recv, target):
        return pltpu.make_async_remote_copy(
            src_ref=src, dst_ref=dst, send_sem=send, recv_sem=recv,
            device_id=target, device_id_type=MESH,
        )

    sibling = device(x, y, z, 1 - c)

    barrier = pltpu.get_barrier_semaphore()

    def greet(target):
        pl.semaphore_signal(barrier, inc=1, device_id=target, device_id_type=MESH)

    for k in (4, 3, 5, 2, 6, 1, 7):
        other = (x * 2 + c + k) % 8
        greet(on_rings((p1 + k) % RING, p2))
        if k in (1, 4, 7):
            greet(on_rings(p1, (p2 + k) % RING))
        greet(device(other // 2, y, z, other % 2))

    def weight_rows(i, path):
        kb, j = i // 4, i % 4
        straight = kb * 768 + j * 192
        across = ((kb % 2) * 4 + j) * 768 + (kb // 2) * 192
        return pl.ds(pl.multiple_of(straight + path * (across - straight), 64), 192)

    def weight_slot(i, k):
        return wk.at[i // 4, pl.ds(pl.multiple_of((i % 4) * 192, 64), 192), pl.ds(pl.multiple_of(k * 128, 128), 128)]

    def local_weights(i, carry):
        rows = weight_rows(i, role)
        pltpu.make_async_copy(gate_ref.at[0, rows, :], weight_slot(i, c), w_sem.at[0]).start()
        pltpu.make_async_copy(up_ref.at[0, rows, :], weight_slot(i, 2 + c), w_sem.at[1]).start()
        return carry

    tok_copy = pltpu.make_async_copy(tok_hbm, tok_ref, in_sem.at[0])
    ids_copy = pltpu.make_async_copy(ids_hbm, ids_ref, in_sem.at[1])
    raw_copy = pltpu.make_async_copy(raw_hbm, raw_ref, in_sem.at[2])
    tok_copy.start()
    ids_copy.start()
    raw_copy.start()
    own_down = dn.at[pl.ds(pl.multiple_of(c * 128, 128), 128), :]
    their_down = dn.at[pl.ds(pl.multiple_of((1 - c) * 128, 128), 128), :]
    pltpu.make_async_copy(down_ref.at[0], own_down, d_sem.at[0]).start()

    lax.fori_loop(0, 32, local_weights, 0)

    ids_copy.wait()
    raw_copy.wait()
    row = lax.broadcasted_iota(jnp.int32, (8, 48), 0)
    weights = raw_ref[...].astype(F32)
    share = weights / (weights[0:1, :] + weights[1:2, :])
    ids = ids_ref[...]
    zero = jnp.zeros((8, 48), F32)
    hit0 = ids[0:1, :] == row
    hit1 = ids[1:2, :] == row
    mix = jnp.where(hit0, share[0:1, :], zero) + jnp.where(hit1, share[1:2, :], zero)
    hits = jnp.where(hit0, 1.0, zero) + jnp.where(hit1, 1.0, zero)
    tabs[z_hi, x, :, 0:48] = mix
    tabs[z_hi, x, :, 48:128] = jnp.where(
        lax.broadcasted_iota(jnp.int32, (8, 80), 1) == 0,
        jnp.sum(hits, axis=1, keepdims=True), jnp.sum(mix, axis=1, keepdims=True),
    )

    tok_copy.wait()
    pl.semaphore_wait(barrier, 17)

    for d in (2, 1, 3):
        remote(
            tok_ref, near.at[x % 2, c], x_send.at[d], x_recv.at[x % 2, c],
            device((x + d) % 4, y, z, (half + y + z) % 2),
        ).start()

    @pl.when(half != role)
    def _():
        remote(tok_ref, near.at[x % 2, c], x_send.at[0], x_recv.at[x % 2, c], sibling).start()

    @pl.when(half == role)
    def _():
        near[x % 2, c] = tok_ref[...]

    table = lambda d: remote(
        tabs.at[z_hi, x], tabs.at[z_hi, x], t_send.at[d], t_recv.at[d],
        device((x + d) % 4, y, z, c),
    )
    for d in (1, 2, 3):
        table(d).start()

    def remote_weights(i, carry):
        rows = weight_rows(i, 1 - role)
        remote(gate_ref.at[0, rows, :], weight_slot(i, c), w_sem.at[2], w_sem.at[4], sibling).start()
        remote(up_ref.at[0, rows, :], weight_slot(i, 2 + c), w_sem.at[3], w_sem.at[5], sibling).start()
        return carry

    down_copy = remote(down_ref.at[0], own_down, d_sem.at[1], d_sem.at[2], sibling)
    down_copy.start()
    lax.fori_loop(0, 32, remote_weights, 0)

    for xh in range(2):
        for cs in range(2):
            @pl.when((2 * role + xh != x) | (c != cs))
            def _():
                remote(
                    tok_ref, near.at[xh, cs], x_send.at[0], x_recv.at[xh, cs], sibling
                ).wait_recv()

    pieces = [near[xh, cs].astype(F32) for xh in range(2) for cs in range(2)]
    first[p1] = jnp.concatenate(pieces, axis=1).astype(BF16)

    around = lambda k: remote(
        first.at[p1], first.at[p1], f_send.at[0], f_recv.at[k], on_rings((p1 + k) % RING, p2)
    )
    for k in (4, 3, 5, 2, 6, 1, 7):
        around(k).start()
    for d in (1, 2, 3):
        remote(
            tabs.at[z_hi, x], tabs.at[z_hi, (x + 4 - d) % 4], t_send.at[d], t_recv.at[d], sibling
        ).wait_recv()
    mirror = device(x, y, (z + 4) % 8, c)
    far_table = remote(tabs.at[z_hi], tabs.at[z_hi], t_send.at[0], t_recv.at[0], mirror)
    far_table.start()

    acc[...] = jnp.zeros_like(acc)

    pair = p1 // 2
    pairs = [pair, (pair + 1) % 4, (pair + 3) % 4, (pair + 2) % 4]

    def near_first(h, rank):
        same = (pair // 2 + h + 1) % 2
        return (pair % 2 + 1 - same + rank) % 2

    def piece(pr, xh):
        return (pr // 2) * 4 + xh * 2 + pr % 2

    pltpu.make_async_copy(down_ref.at[0], own_down, d_sem.at[0]).wait()
    pltpu.make_async_copy(down_ref.at[0], their_down, d_sem.at[2]).wait()

    @pl.when(role == 0)
    def _():
        for kb in range(8):
            dk[kb] = dn[:, kb * 768:(kb + 1) * 768]

    @pl.when(role == 1)
    def _():
        def repack(g, carry):
            rows = pl.ds(pl.multiple_of(g * 32, 32), 32)
            for kb in range(8):
                lo, hi = kb // 2, kb % 2
                cuts = [
                    dn[rows, (hi * 4 + j) * 768 + lo * 192:(hi * 4 + j) * 768 + (lo + 1) * 192].astype(F32)
                    for j in range(4)
                ]
                dk[kb, rows, :] = jnp.concatenate(cuts, axis=1).astype(BF16)
            return carry

        lax.fori_loop(0, 8, repack, 0)

    def ring_copy(way, step, b, sub):
        target = on_rings(p1, (p2 + (1 if way == 0 else 7)) % RING)
        return remote(
            blocks.at[b, sub], blocks.at[b, sub],
            a_send.at[0], a_recv.at[way, step * 8 + sub - step // 3 * way * 4], target,
        )

    def first_come(source):
        k = (p1 + RING - source) % RING
        remote(first.at[p1], first.at[source], f_send.at[0], f_recv.at[k], sibling).wait_recv()

    for j in range(4):
        if j == 0:
            first_come(p1 + 1 - 2 * (p1 % 2))
        else:
            first_come(pairs[j] * 2)
            first_come(pairs[j] * 2 + 1)
        for xh in range(2):
            sub = piece(pairs[j], xh)
            parts = [
                first[pairs[j] * 2 + lo][:, xh * 192:(xh + 1) * 192].astype(F32) for lo in range(2)
            ]
            blocks[p2, sub] = jnp.concatenate(parts, axis=1).astype(BF16)
            ring_copy(0, 0, p2, sub).start()
            ring_copy(1, 0, p2, sub).start()

    def place(b, h):
        across = (b % 4) * 2 + h
        return b + role * (across - b), h + role * (b // 4 - h)

    def project(b, h):
        kb, r = place(b, h)
        part = blocks[b, pl.ds(4 * h, 4)]
        rows = jnp.concatenate(
            [jnp.concatenate([part[2 * xh], part[2 * xh + 1]], axis=1) for xh in range(2)], axis=0
        )
        acc[r] += jnp.dot(rows, wk[kb], preferred_element_type=F32)

    def weights_here():
        for k in range(2):
            mine = wk.at[:, :, pl.ds(pl.multiple_of((2 * k + c) * 128, 128), 128)]
            theirs = wk.at[:, :, pl.ds(pl.multiple_of((2 * k + 1 - c) * 128, 128), 128)]
            pltpu.make_async_copy(mine, mine, w_sem.at[k]).wait()
            pltpu.make_async_copy(theirs, theirs, w_sem.at[4 + k]).wait()

    def gather_step(r, carry):
        held = ((p2 + RING - r) % RING, (p2 + r) % RING)
        before = ((p2 + RING + 1 - r) % RING, (p2 + r - 1) % RING)
        for j in range(4):
            h = pairs[j] // 2
            for xh in range(2):
                sub = piece(pairs[j], xh)
                for way in range(2):
                    ring_copy(way, r - 1, held[way], sub).wait_recv()

                    @pl.when((r < 3) | (h == way))
                    def _():
                        ring_copy(way, r, held[way], sub).start()

                if xh == 0 and j == 0:
                    pl.when(r == 1)(weights_here)
                if xh == 0 and j % 2 == 0:
                    project(before[0], j // 2)
                elif xh == 0:
                    @pl.when(r > 1)
                    def _():
                        project(before[1], j // 2)
        return carry

    lax.fori_loop(1, 4, gather_step, 0)
    remote(tabs.at[z_hi], tabs.at[1 - z_hi], t_send.at[0], t_recv.at[0], mirror).wait_recv()
    lane96 = lax.broadcasted_iota(jnp.int32, (128, 8), 1)
    for r in range(2):
        for xh in range(2):
            turned = jnp.transpose(tabs[r, 2 * role + xh])
            picked = jnp.sum(jnp.where(lane96 == e, turned, 0.0), axis=1, keepdims=True)
            scl[r, xh * 48:(xh + 1) * 48, :] = jnp.broadcast_to(picked[0:48], (48, 128))
    everyone = tabs[0, 0]
    for k in range(1, 8):
        everyone = everyone + tabs[k // 4, k % 4]
    load_ref[...] = jnp.transpose(everyone)[48:50, :] / 48.0

    far = (p2 + 4) % RING
    for rank in range(2):
        for xh in range(2):
            for way in range(2):
                sub = way * 4 + xh * 2 + near_first(way, rank)
                ring_copy(way, 3, far, sub).wait_recv()
            project((p2 + (5 if xh == 0 else 3)) % RING, rank)
    for way in range(2):
        project(far, way)

    for r in range(2):
        gate = acc[r, :, 0:256]
        up = acc[r, :, 256:512]
        hid[r] = (gate / (1.0 + jnp.exp(-gate)) * up).astype(BF16)

    def own_part(q, h):
        kb, r = place(q, h)
        part = jnp.dot(hid[r], dk[kb], preferred_element_type=F32)
        return part * scl[r][:, 0:1]

    def sum_copy(way, s, sub):
        target = on_rings(p1, (p2 + (1 if way == 0 else 7)) % RING)
        return remote(
            sent.at[way, s, sub], came.at[way, s, sub],
            r_send.at[0], r_recv.at[way, (s * 8 + sub - 4) if s is not None and not isinstance(s, int) else (sub - way * 4 if s == 0 else s * 8 + sub - 4)], target,
        )

    def prepare(s, k, way):
        q = (p2 + (4 - s if way == 0 else 4 + s)) % RING
        part = own_part(q, 1 - way if k == 0 else way)
        for xh in range(2):
            for lh in range(2):
                ahead[way, k, xh, lh] = part[xh * 48:(xh + 1) * 48, lh * 384:(lh + 1) * 384]

    def pass_on(s, k, has_come, following=None):
        for i in range(4):
            xh = i % 2
            for way in range(2):
                h = 1 - way if k == 0 else way
                lh = near_first(h, 1 - i // 2)
                sub = h * 4 + xh * 2 + lh
                value = ahead[way, k, xh, lh]
                if has_come:
                    sum_copy(way, s - 1, sub).wait_recv()
                    value = value + came[way, s - 1, sub].astype(F32)
                sent[way, s, sub] = value.astype(BF16)
                sum_copy(way, s, sub).start()
            if following is not None and i % 2 == 0:
                prepare(*following, i // 2)

    for way in range(2):
        prepare(0, 1, way)
    pass_on(0, 1, False, (1, 0))
    pass_on(1, 0, False)
    for way in range(2):
        prepare(1, 1, way)
    pass_on(1, 1, True, (2, 0))

    def sum_step(s, carry):
        pass_on(s, 0, True, (s, 1))
        pass_on(s, 1, True, (s + 1, 0))
        return carry

    lax.fori_loop(2, 4, sum_step, 0)

    def scatter(target):
        k = (target + RING - p1) % RING
        return remote(
            own16.at[target], direct.at[k], l_send.at[0], l_recv.at[k], on_rings(target, p2)
        )

    def scatter_pair(pr):
        for lo in range(2):
            target = pr * 2 + lo

            @pl.when(target != p1)
            def _():
                scatter(target).start()

    for rank in (1, 0):
        for h in range(2):
            lh = near_first(h, rank)
            halves = []
            for xh in range(2):
                sub = h * 4 + xh * 2 + lh
                value = ahead[1 - h, 0, xh, lh]
                for way in (1 - h, h):
                    sum_copy(way, 3, sub).wait_recv()
                    value = value + came[way, 3, sub].astype(F32)
                halves.append(value)
            for lo in range(2):
                both = jnp.concatenate([v[:, lo * 192:(lo + 1) * 192] for v in halves], axis=1)
                own32[h * 4 + lh * 2 + lo] = both
                own16[h * 4 + lh * 2 + lo] = both.astype(BF16)

            scatter_pair(h * 2 + lh)

    for d in (1, 2, 3):
        table(d).wait_send()
        remote(
            tok_ref, near.at[x % 2, c], x_send.at[d], x_recv.at[x % 2, c],
            device((x + d) % 4, y, z, (half + y + z) % 2),
        ).wait_send()

    @pl.when(half != role)
    def _():
        remote(tok_ref, near.at[x % 2, c], x_send.at[0], x_recv.at[x % 2, c], sibling).wait_send()

    far_table.wait_send()
    down_copy.wait_send()
    for k in range(2):
        mine = wk.at[:, :, pl.ds(pl.multiple_of((2 * k + c) * 128, 128), 128)]
        pltpu.make_async_copy(mine, mine, w_sem.at[2 + k]).wait()

    for sem, kept in ((f_send, first), (a_send, blocks), (r_send, blocks)):
        gone = kept.at[pl.ds(0, 7)]
        pltpu.make_async_copy(gone, gone, sem.at[0]).wait()
    total = own32[p1]
    for k in (1, 7, 2, 6, 3, 5, 4):
        remote(own16.at[0], direct.at[k], l_send.at[0], l_recv.at[k], sibling).wait_recv()
        total = total + direct[k].astype(F32)
    for xt in range(2):
        for ct in range(2):
            last_out[xt, ct] = total[:, xt * 192 + ct * 96:xt * 192 + (ct + 1) * 96]

    def home(xt, ct):
        return remote(
            last_out.at[xt, ct], last_in.at[x], o_send.at[xt, ct], o_recv.at[x],
            device(2 * role + xt, y, z, ct),
        )

    for rank in range(2):
        for ct in range(2):
            xt = (x + rank) % 2

            @pl.when((2 * role + xt != x) | (c != ct))
            def _():
                home(xt, ct).start()

    @pl.when(half == role)
    def _():
        last_in[x] = last_out[x % 2, c]

    for xs in range(4):
        @pl.when((xs != x) | (half != role))
        def _():
            remote(
                last_out.at[0, 0], last_in.at[xs], o_send.at[0, 0], o_recv.at[xs], sibling
            ).wait_recv()
    out_ref[...] = (last_in[0] + last_in[1] + last_in[2] + last_in[3]).astype(BF16)
    for xt in range(2):
        for ct in range(2):
            @pl.when((2 * role + xt != x) | (c != ct))
            def _():
                home(xt, ct).wait_send()
    gone = own16.at[pl.ds(0, 7)]
    pltpu.make_async_copy(gone, gone, l_send.at[0]).wait()


def hand_out(mixed_ref, load_ref, mixed_out, load_out, sem):
    copies = [
        pltpu.make_async_copy(mixed_ref, mixed_out, sem.at[0]),
        pltpu.make_async_copy(load_ref, load_out, sem.at[1]),
    ]
    for copy in copies:
        copy.start()
    for copy in copies:
        copy.wait()


def local(tokens, expert_ids, route_weight, gate_weight, up_weight, down_weight):
    vmem, dma = pltpu.VMEM, pltpu.SemaphoreType.DMA
    inside = pl.BlockSpec(memory_space=pltpu.VMEM)
    outside = pl.BlockSpec(memory_space=pltpu.HBM)
    shapes = (jax.ShapeDtypeStruct((48, 96), BF16), jax.ShapeDtypeStruct((2, 8), F32))
    result = pl.pallas_call(
        kernel,
        name="layer",
        out_shape=(
            jax.ShapeDtypeStruct((48, 96), BF16),
            jax.ShapeDtypeStruct((2, 8), F32),
        ),
        in_specs=[outside] * 6,
        out_specs=(inside, inside),
        scratch_shapes=[
            vmem((48, 96), BF16),
            vmem((2, 48), jnp.int32),
            vmem((2, 48), jnp.int32),
            vmem((2, 2, 48, 96), BF16),
            vmem((2, 4, 8, 128), F32),
            vmem((8, 48, 384), BF16),
            vmem((8, 8, 48, 384), BF16),
            vmem((8, 768, 512), BF16),
            vmem((256, 6144), BF16),
            vmem((8, 256, 768), BF16),
            vmem((2, 96, 512), F32),
            vmem((2, 96, 256), BF16),
            vmem((2, 96, 128), F32),
            vmem((2, 2, 2, 2, 48, 384), F32),
            vmem((2, 4, 8, 48, 384), BF16),
            vmem((2, 4, 8, 48, 384), BF16),
            vmem((8, 48, 384), F32),
            vmem((8, 48, 384), BF16),
            vmem((8, 48, 384), BF16),
            vmem((2, 2, 48, 96), F32),
            vmem((4, 48, 96), F32),
            dma((3,)),
            dma((6,)),
            dma((3,)),
            dma((4,)),
            dma((2, 2)),
            dma((4,)),
            dma((4,)),
            dma((1,)),
            dma((8,)),
            dma((1,)),
            dma((2, 28)),
            dma((1,)),
            dma((2, 28)),
            dma((1,)),
            dma((8,)),
            dma((2, 2)),
            dma((4,)),
        ],
        compiler_params=pltpu.CompilerParams(
            collective_id=0, has_side_effects=True, vmem_limit_bytes=48 * 1024 * 1024
        ),
    )(*[
        pltpu.with_memory_space_constraint(a, pltpu.HBM)
        for a in (tokens, expert_ids.T, route_weight.T, gate_weight, up_weight, down_weight)
    ])
    return pl.pallas_call(
        hand_out,
        name="hand_out",
        out_shape=shapes,
        in_specs=[inside] * 2,
        out_specs=(outside, outside),
        scratch_shapes=[dma((2,))],
        compiler_params=pltpu.CompilerParams(vmem_limit_bytes=1024 * 1024),
    )(*result)


def solution(mesh):
    placed = (
        P("expert", "tensor"),
        P("expert", None),
        P("expert", None),
        P("expert", None, "tensor"),
        P("expert", None, "tensor"),
        P("expert", "tensor", None),
    )
    return jax.shard_map(
        local, mesh=mesh, in_specs=placed, out_specs=(P("expert", "tensor"), P()), check_vma=False
    )
```
